32 devices in a mesh: front: 8 (over y, x, core), sub: 4 (over z).
Axes of the slice: x: 2, y: 2, z: 4, core: 2. Of those that a mesh axis runs over, the one named last changes fastest.
Arguments:
- row_values: float32 [4096, 1024], P(('front', 'sub')), may hold values from -0.12 to 0.12
- front_of_row: int32 [4096, 1], P(('front', 'sub')), may hold values from 0 to 7; in each aligned block of 128 rows (0 to 127, 128 to 255, ...) at most 32 rows name the same one
- child_factors: float32 [16, 512, 512], P('front', 'sub'), as said below
- child_columns: int32 [16, 512], P('front'), may hold values from 0 to 1023, as said below
- damping: float32 [8, 1024], P('front'), may hold values from 0.5 to 2
Outputs:
- front_factor: float32 [8, 1024, 1024], P('front', 'sub')
The draws below stay inside these ranges and needn't reach their ends.
Inputs may be any that keep to these rules, and one draw needn't show every extreme that they name: `front_of_row`: among the 128 rows of one device, at most 32 name the same front, and some device's block reaches this bound. `child_factors`: each block is upper triangular with a positive diagonal. `child_columns`: each row names 512 distinct columns.
All inputs are finite; a program needn't handle non-finite values.
Results may differ from the reference program's by a relative error of at most 0.0003.
Values sent between devices are 32-bit elements; how exact they have to be, the bound alone decides.
A program may use at most 64 MiB of HBM per device.

```python
import math
import jax
import jax.numpy as jnp
import numpy as np
from jax import lax

CONTRIB = 512
F = 1024
ROWS_SRC = 128
FRONTS = 8
MOST = 32
ROWS = 4096
N_FRONT = 8
N_SUB = 4


def draw_child_factors(key, part):
    key_diag = jax.random.fold_in(key, 11)
    key_off = jax.random.fold_in(key, 12)
    shape = (2 * FRONTS, CONTRIB, CONTRIB)
    diagonal = jnp.exp(jax.random.uniform(key_diag, (2 * FRONTS, CONTRIB), jnp.float32, jnp.log(0.5), jnp.log(2.0)))
    offdiag = jnp.clip(jax.random.normal(key_off, shape, jnp.float32), -5.0, 5.0) * (0.5 / jnp.sqrt(jnp.float32(CONTRIB)))
    upper_mask = jnp.triu(jnp.ones((CONTRIB, CONTRIB), jnp.float32), 1)
    eye_mask = jnp.eye(CONTRIB, dtype=jnp.float32)
    return (offdiag * upper_mask[None] + diagonal[:, :, None] * eye_mask[None]).astype(jnp.float32)


def draw_child_columns(key, part):
    key_score = jax.random.fold_in(key, 21)
    scores = jax.random.randint(key_score, (2 * FRONTS, F), 0, 2 ** 19, jnp.int32)
    distinct = scores * F + jnp.arange(F, dtype=jnp.int32)[None, :]
    permuted = jnp.argsort(distinct, axis=1, stable=True).astype(jnp.int32)
    return permuted[:, :CONTRIB]


def level_of(key, extent, cuts, low, largest):
    gain = 1.0
    for position, parts in cuts:
        steps = jax.random.uniform(jax.random.fold_in(jax.random.fold_in(key, 6), position), (parts,), jnp.float32, low / len(cuts), largest / len(cuts))
        gain = gain * jnp.repeat(jnp.exp(steps), extent[position] // parts).reshape((-1,) + (1,) * (len(extent) - 1 - position))
    return gain


def shared_out(stream_key, own, number, rows, number_of, top, reach, skew):
    order = jax.random.permutation(stream_key, number_of)
    crowded, usual = load_shares(number_of, rows * top, reach, skew, True), load_shares(number_of, rows * top, reach, skew, False)
    places = jnp.arange(number_of)

    def named(tallies, rotation):
        used = int((tallies > 0).sum())
        fixed = max(1, used // 4)
        passed = fixed + (places - fixed + rotation * (used - fixed)) % max(1, number_of - fixed)
        return jnp.zeros((number_of,), jnp.int32).at[order[jnp.where(places < fixed, places, passed)]].set(jnp.asarray(tallies, jnp.int32))

    tallies = jnp.where(number % 4 == 0, named(crowded, number // 4), named(usual, number - number // 4 - 1))
    mixed = jax.random.permutation(jax.random.fold_in(own, 3), number_of)
    giver, taker = mixed[0:number_of // 2 * 2:2], mixed[1:number_of // 2 * 2:2]
    slack = jnp.minimum(tallies[giver] - 1, reach - tallies[taker]) // 2
    slack = jnp.where((giver == order[0]) | (taker == order[0]) | (tallies[taker] == 0), 0, jnp.maximum(slack, 0))
    passed = jax.random.randint(jax.random.fold_in(own, 4), (number_of // 2,), 0, 1 << 20) % (slack + 1)
    tallies = tallies.at[giver].add(-passed).at[taker].add(passed)
    items = jnp.searchsorted(jnp.cumsum(tallies), jnp.arange(rows * top), side="right").astype(jnp.int32)
    listing = items.reshape(top, rows).T
    listing = listing[jax.random.permutation(jax.random.fold_in(own, 1), rows)]
    rotation = jax.random.randint(jax.random.fold_in(own, 2), (rows, 1), 0, top)
    return jnp.take_along_axis(listing, (jnp.arange(top)[None, :] + rotation) % top, axis=1)


def load_shares(number_of, total, limit, slope, full):
    portions = [(1 << 20) // math.isqrt(rank ** slope) + 1 for rank in range(1, number_of + 1)]
    largest = limit if full else min(limit, max(-(-total // number_of), total * portions[0] // sum(portions)))
    least = 1 if total - largest >= number_of - 1 else 0
    holding, spare = [largest] + [least] * (number_of - 1), total - largest - least * (number_of - 1)
    while spare > 0:
        free = [i for i in range(1, number_of) if holding[i] < largest] or [i for i in range(1, number_of) if holding[i] < limit]
        pool, remaining = sum([portions[i] for i in free]), spare
        for i in free:
            addition = min(limit - holding[i], max(1, remaining * portions[i] // pool), spare)
            holding[i] = holding[i] + addition
            spare = spare - addition
    return np.array(holding)


def noise(rng, extent, scale, limit, pieces=(), held_as=jnp.bfloat16):
    level = level_of(rng, extent, pieces, -0.22, 0.18) if pieces else 1.0
    values = jax.random.normal(rng, extent, jnp.float32) * scale * level
    return jnp.minimum(jnp.maximum(values, -limit), limit).astype(held_as)


def setup_inputs(seed: int = 0) -> dict:
    key_list = jax.random.split(jax.random.key(seed), 6)
    row_values = noise(key_list[0], (ROWS, F), 0.02, 0.12, ((0, 32),), jnp.float32)
    front_of_row_keys = jax.random.split(jax.random.fold_in(key_list[1], 1), ROWS // ROWS_SRC)
    front_of_row_turns = jax.random.permutation(jax.random.fold_in(key_list[1], 3), ROWS // ROWS_SRC)
    front_of_row = jax.vmap(lambda own, number: shared_out(jax.random.fold_in(key_list[1], 2), own, number, ROWS_SRC, FRONTS, 1, MOST, 2))(front_of_row_keys, front_of_row_turns).reshape((ROWS, 1))
    child_factors = draw_child_factors(jax.random.fold_in(key_list[5], 71), 0)
    child_columns = draw_child_columns(jax.random.fold_in(key_list[5], 71), 0)
    damping = jnp.clip(jnp.exp(math.log(2.0) - 1.3862944 * jax.random.uniform(key_list[4], (FRONTS, F), jnp.float32) ** level_of(key_list[4], (FRONTS, F), ((0, 8),), -0.2, 0.2)), 0.5, 2.0)
    return {"row_values": row_values, "front_of_row": front_of_row, "child_factors": child_factors, "child_columns": child_columns, "damping": damping}


HIGHEST = lax.Precision.HIGHEST

def gram_product(matrix):
    return lax.dot_general(matrix.astype(jnp.float32), matrix.astype(jnp.float32), (((0,), (0,)), ((), ())), precision=HIGHEST, preferred_element_type=jnp.float32)

def reference(row_values, front_of_row, child_factors, child_columns, damping):
    destination = front_of_row[:, 0].astype(jnp.int32)
    sorted_rows = jnp.argsort(destination, stable=True).astype(jnp.int32)
    counts = jnp.bincount(destination, length=FRONTS).astype(jnp.int32)
    starts = (jnp.cumsum(counts) - counts).astype(jnp.int32)
    capacity = MOST * N_FRONT * N_SUB
    padded_order = jnp.concatenate([sorted_rows, jnp.zeros((capacity,), jnp.int32)])
    columns = jnp.arange(F, dtype=jnp.int32)

    def factor_front(front_index):
        row_index = lax.dynamic_slice(padded_order, (starts[front_index],), (capacity,))
        is_live = jnp.arange(capacity, dtype=jnp.int32) < counts[front_index]
        front_rows = jnp.where(is_live[:, None], row_values[row_index], jnp.float32(0.0))
        gram_matrix = gram_product(front_rows)
        for child_index in range(2):
            child = child_factors[2 * front_index + child_index]
            mapping = child_columns[2 * front_index + child_index]
            spread = (mapping[:, None] == columns[None, :]).astype(jnp.float32)
            placed = jnp.dot(child.astype(jnp.float32), spread.astype(jnp.float32), precision=HIGHEST, preferred_element_type=jnp.float32)
            gram_matrix = gram_matrix + gram_product(placed)
        weight = damping[front_index]
        gram_matrix = gram_matrix + jnp.diag(weight * weight)
        return jnp.linalg.cholesky(gram_matrix).T
    return lax.map(factor_front, jnp.arange(FRONTS, dtype=jnp.int32))
```

```python
import functools
import jax, jax.numpy as jnp
from jax import lax
from jax.experimental import pallas as pl
from jax.experimental.pallas import tpu as pltpu
from jax.sharding import PartitionSpec as P

NB = 128
CW = 2 * NB
BF = jnp.bfloat16
F32 = jnp.float32


def split3(x):
    h = x.astype(BF)
    r = x - h.astype(F32)
    m = r.astype(BF)
    l = (r - m.astype(F32)).astype(BF)
    return h, m, l


def split2(x):
    h = x.astype(BF)
    return h, (x - h.astype(F32)).astype(BF)


def tdot(a, b):
    return lax.dot_general(a, b, (((0,), (0,)), ((), ())), preferred_element_type=F32)


def mm(a, b):
    return lax.dot_general(a, b, (((1,), (0,)), ((), ())), preferred_element_type=F32)


def factor_diag(m_ref, B, slot):
    for b in range(NB // B):
        lo = b * B
        slot(b)
        rows = m_ref[lo:lo + B, :]
        sub = lax.broadcasted_iota(jnp.int32, (B, 1), 0)
        cs = [jnp.broadcast_to(rows[:, lo + j:lo + j + 1], (B, NB)) for j in range(B)]
        for j in range(B):
            c = cs[j]
            r = lax.rsqrt(c[j:j + 1, :])
            mult = jnp.where(sub > j, c * r, 0.0)
            r2 = jnp.concatenate([r, r], axis=1)
            pivot = rows[j:j + 1, :] * r2
            m2 = jnp.concatenate([mult, mult], axis=1)
            rows = jnp.where(sub == j, pivot, rows - m2 * pivot)
            for i in range(j + 1, B):
                cs[i] = cs[i] - mult * (cs[i][j:j + 1, :] * r)
        m_ref[lo:lo + B, :] = rows
        if lo + B < NB:
            h, m, l = split3(rows)
            left = jnp.concatenate([h, h, m, h, l, m], axis=0)[:, :NB]
            right = jnp.concatenate([h, m, h, l, h, m], axis=0)
            upd = tdot(left, right)
            m_ref[lo + B:, :] = m_ref[lo + B:, :] - upd[lo + B:, :]


MESH = pl.DeviceIdType.MESH


def dot3(lhs, h, l):
    return mm(lhs, jnp.concatenate([h, l, h], axis=0))


def left3(h, l):
    return jnp.concatenate([h, h, l], axis=1)


def fused_body(n, fronts, cap, B, x_ref, d_ref, ch_ref, cc_ref, w_ref, o_ref, out_ref, in_ref, fs, fg, a_ref, m_ref, rt_ref, rr_ref, tt_ref, xh_ref, xl_ref, th_ref, tl_ref, p_ref, l_ref, f_ref, ss, sg, os, og):
    R, F = x_ref.shape
    kids, crows, _ = ch_ref.shape
    slots = fronts * cap
    panels = F // NB
    chunks = F // CW
    per = panels // n
    me = lax.axis_index("sub")
    mine = lax.axis_index("front")
    side = lax.rem(mine, 2)
    pos = me + side * (n - 1 - 2 * me)
    top = (n - 1) * (1 - side)
    step = 1 - 2 * side
    is_root = pos == n - 1
    is_first = pos == 0

    barrier = pltpu.get_barrier_semaphore()

    def greet_sub(k, c):
        pl.semaphore_signal(barrier, inc=1, device_id={"sub": lax.rem(me + k, n)}, device_id_type=MESH)
        return c

    def greet_front(k, c):
        pl.semaphore_signal(barrier, inc=1, device_id={"front": lax.rem(mine + k, fronts)}, device_id_type=MESH)
        return c

    lax.fori_loop(1, n, greet_sub, 0)
    lax.fori_loop(1, fronts, greet_front, 0)

    def cols_of(c):
        return pl.ds(pl.multiple_of(c * CW, CW), CW)

    def rows_of(f):
        return pl.ds(pl.multiple_of(f * cap, cap), cap)

    def post(k, c, dst_front):
        to = lax.rem(mine + k, fronts)
        return pltpu.make_async_remote_copy(
            src_ref=out_ref.at[c, rows_of(to)], dst_ref=in_ref.at[c, rows_of(dst_front)], send_sem=fs.at[c, k],
            recv_sem=fg.at[c, k], device_id={"front": to}, device_id_type=MESH)

    dest = d_ref[...]
    hot = dest == lax.broadcasted_iota(jnp.int32, (R, fronts), 1)
    below = lax.broadcasted_iota(jnp.int32, (R, R), 1) < lax.broadcasted_iota(jnp.int32, (R, R), 0)
    before = mm(below.astype(F32).astype(BF), hot.astype(F32).astype(BF))
    position = jnp.sum(jnp.where(hot, before, 0.0), axis=1, keepdims=True)
    slot_of = dest.astype(F32) * cap + position
    pick = (slot_of == lax.broadcasted_iota(jnp.int32, (R, slots), 1).astype(F32)).astype(F32).astype(BF)
    pick2 = jnp.concatenate([pick, pick], axis=0).T

    def route(c):
        out_ref[c] = mm(pick2, jnp.concatenate(split2(x_ref[:, cols_of(c)]), axis=0))

    def post_rows(c):
        def one(k, cc):
            post(k, c, mine).start()
            return cc

        lax.fori_loop(1, fronts, one, 0)
        in_ref[c, rows_of(mine), :] = out_ref[c, rows_of(mine), :]

    route(0)
    pl.semaphore_wait(barrier, fronts + n - 2)
    post_rows(0)

    def route_rest(c, cc):
        route(c)
        post_rows(c)
        return cc

    lax.fori_loop(1, chunks, route_rest, 0)

    def place_kids(c, cc):
        for kid in range(kids):
            h, l = split2(ch_ref[kid])
            spread = (lax.broadcasted_iota(jnp.int32, (CW, cc_ref.shape[1]), 0) + c * CW == cc_ref[kid:kid + 1, :]).astype(F32).astype(BF)
            both = lax.dot_general(jnp.concatenate([h, l], axis=0), spread, (((1,), (1,)), ((), ())), preferred_element_type=F32)
            xh_ref[c, kid * crows:(kid + 1) * crows, :] = both[:crows].astype(BF)
            xl_ref[c, kid * crows:(kid + 1) * crows, :] = both[crows:].astype(BF)
        return cc

    lax.fori_loop(0, chunks, place_kids, 0)

    def place(i, j):
        return j * (j + 1) // 2 + i

    def hop(src, c):
        return pltpu.make_async_remote_copy(
            src_ref=src.at[c], dst_ref=l_ref.at[c], send_sem=ss.at[c], recv_sem=sg.at[c],
            device_id={"sub": lax.rem(me + step + n, n)}, device_id_type=MESH)

    def stream(c):
        @pl.when(is_first)
        def _():
            hop(p_ref, c).start()

        @pl.when((pos > 0) & (pos < n - 1))
        def _():
            hop(f_ref, c).wait_recv()
            f_ref[c] = l_ref[c] + p_ref[c]
            hop(f_ref, c).start()

    def gram_chunk(J, carry):
        def take(k, cc):
            post(k, J, lax.rem(mine + fronts - k, fronts)).wait_recv()
            return cc

        lax.fori_loop(1, fronts, take, 0)
        h, l = split2(in_ref[J])
        xh_ref[J, kids * crows:, :] = h
        xl_ref[J, kids * crows:, :] = l
        th_ref[J] = xh_ref[J].T
        tl_ref[J] = xl_ref[J].T

        def gram_block(I, cc):
            block = dot3(left3(th_ref[I], tl_ref[I]), xh_ref[J], xl_ref[J])
            i, j = 2 * I, 2 * J
            p_ref[place(i, j)] = block[:NB, :NB]
            p_ref[place(i, j + 1)] = block[:NB, NB:]
            p_ref[place(i + 1, j + 1)] = block[NB:, NB:]

            @pl.when(J > I)
            def _():
                p_ref[place(i + 1, j)] = block[NB:, :NB]

            stream(place(i, j))
            stream(place(i, j + 1))

            @pl.when(J > I)
            def _():
                stream(place(i + 1, j))

            stream(place(i + 1, j + 1))
            return cc

        return lax.fori_loop(0, J + 1, gram_block, carry)

    lax.fori_loop(0, chunks, gram_chunk, 0)

    ri = lax.broadcasted_iota(jnp.int32, (NB, NB), 0)
    ci = lax.broadcasted_iota(jnp.int32, (NB, NB), 1)

    def at(i, j):
        return (pl.ds(pl.multiple_of(i * NB, NB), NB), pl.ds(pl.multiple_of(j * NB, NB), NB))

    def at2(i, j):
        return (pl.ds(pl.multiple_of(i * CW, CW), CW), pl.ds(pl.multiple_of(j * CW, CW), CW))

    def ship(i, j):
        c = place(i, j)
        owner = i // per
        return pltpu.make_async_remote_copy(
            src_ref=a_ref.at[at(i, j)], dst_ref=o_ref.at[at(i - owner * per, j)], send_sem=os.at[c], recv_sem=og.at[c],
            device_id={"sub": owner}, device_id_type=MESH)

    def emit(i, j):
        @pl.when(i // per == me)
        def _():
            o_ref[at(i - me * per, j)] = a_ref[at(i, j)]

        @pl.when(i // per != me)
        def _():
            ship(i, j).start()

    def serve(i, j):
        c = place(i, j)
        hop(p_ref, c).wait_recv()
        a_ref[at(i, j)] = p_ref[c] + l_ref[c]

        @pl.when(i == j)
        def _():
            wt = w_ref[:, pl.ds(pl.multiple_of(i * NB, NB), NB)]
            a_ref[at(i, j)] += jnp.where(ri == ci, wt * wt, 0.0)

    def factor(p):
        m_ref[:, :NB] = a_ref[at(p, p)]
        m_ref[:, NB:] = (ri == ci).astype(F32)
        factor_diag(m_ref, B, lambda b: None)
        a_ref[at(p, p)] = jnp.where(ci >= ri, m_ref[:, :NB], 0.0)
        emit(p, p)
        return jnp.where(ci <= ri, m_ref[:, NB:], 0.0)

    def keep_t(P, r0, c0, t):
        h, l = split2(t)
        tt_ref[P, r0:r0 + NB, c0:c0 + NB] = h
        tt_ref[P, r0:r0 + NB, CW + c0:CW + c0 + NB] = h
        tt_ref[P, r0:r0 + NB, 2 * CW + c0:2 * CW + c0 + NB] = l

    def supercolumn(P, carry):
        for j in (2 * P, 2 * P + 1):
            def col(i, cc):
                serve(i, j)
                return cc
            lax.fori_loop(0, j + 1, col, 0)
        a_ref[at(2 * P + 1, 2 * P)] = jnp.zeros((NB, NB), F32)

        def solve(Q, cc):
            h, l = split2(a_ref[at2(Q, P)])
            r = dot3(tt_ref[Q], h, l)
            a_ref[at2(Q, P)] = r
            for i in range(2):
                for j in range(2):
                    emit(2 * Q + i, 2 * P + j)
            h, l = split2(r)
            rr_ref[...] = jnp.concatenate([h, l, h], axis=0)
            rt_ref[Q, P] = left3(h.T, l.T)

            def update(I, c3):
                a_ref[at2(I, P)] -= mm(rt_ref[Q, I], rr_ref[...])
                return c3

            return lax.fori_loop(Q + 1, P + 1, update, cc)

        lax.fori_loop(0, P, solve, 0)

        p = 2 * P
        t0 = factor(p)
        h, l = split2(a_ref[at(p, p + 1)])
        th, tl = split2(t0)
        r = dot3(left3(th, tl), h, l)
        a_ref[at(p, p + 1)] = r
        emit(p, p + 1)
        h, l = split2(r)
        rl = left3(h.T, l.T)
        a_ref[at(p + 1, p + 1)] -= dot3(rl, h, l)
        keep_t(P, 0, 0, t0)
        keep_t(P, 0, NB, jnp.zeros((NB, NB), F32))
        m2 = dot3(rl, th, tl)
        rr_ref[:NB, :NB], rr_ref[NB:CW, :NB] = split2(m2)
        t1 = factor(p + 1)
        keep_t(P, NB, NB, t1)
        th, tl = split2(t1)
        keep_t(P, NB, 0, -dot3(left3(th, tl), rr_ref[:NB, :NB], rr_ref[NB:CW, :NB]))
        return carry

    def over_blocks(row_lo, row_hi, fn):
        def row(i, c):
            def one(j, cc):
                fn(i, j)
                return cc
            return lax.fori_loop(i, panels, one, c)
        lax.fori_loop(row_lo, row_hi, row, 0)

    def blank(i, c):
        def one(j, cc):
            o_ref[at(i, j)] = jnp.zeros((NB, NB), F32)
            return cc
        return lax.fori_loop(0, me * per + i, one, c)

    lax.fori_loop(0, per, blank, 0)

    @pl.when(is_root)
    def _():
        lax.fori_loop(0, chunks, supercolumn, 0)

        def sent(i, j):
            @pl.when(i // per != me)
            def _():
                ship(i, j).wait_send()
        over_blocks(0, panels, sent)

    @pl.when(jnp.logical_not(is_root))
    def _():
        over_blocks(me * per, me * per + per, lambda i, j: ship(i, j).wait_recv())

        def sent(c, cc):
            hop(f_ref, c).wait_send()
            return cc
        lax.fori_loop(0, panels * (panels + 1) // 2, sent, 0)

    def sent_rows(c, cc):
        def one(k, c3):
            post(k, c, mine).wait_send()
            return c3
        return lax.fori_loop(1, fronts, one, cc)

    lax.fori_loop(0, chunks, sent_rows, 0)


def local(row_values, front_of_row, child_factors, child_columns, damping, B=16):
    fronts, n = lax.axis_size("front"), lax.axis_size("sub")
    rows_held, F = row_values.shape
    cap = -(-(2 * rows_held // fronts) // 8) * 8
    K = fronts * cap + child_factors.shape[0] * child_factors.shape[1]
    panels, chunks = F // NB, F // CW
    total = panels * (panels + 1) // 2
    DMA = pltpu.SemaphoreType.DMA
    return pl.pallas_call(
        functools.partial(fused_body, n, fronts, cap, B),
        out_shape=jax.ShapeDtypeStruct((F // n, F), F32),
        in_specs=[pl.BlockSpec(memory_space=pltpu.VMEM)] * 5,
        out_specs=pl.BlockSpec(memory_space=pltpu.VMEM),
        scratch_shapes=[
            pltpu.VMEM((chunks, fronts * cap, CW), F32),
            pltpu.VMEM((chunks, fronts * cap, CW), F32),
            DMA((chunks, fronts)),
            DMA((chunks, fronts)),
            pltpu.VMEM((F, F), F32),
            pltpu.VMEM((NB, 2 * NB), F32),
            pltpu.VMEM((chunks, chunks, CW, 3 * CW), BF),
            pltpu.VMEM((3 * CW, CW), BF),
            pltpu.VMEM((chunks, CW, 3 * CW), BF),
            pltpu.VMEM((chunks, K, CW), BF),
            pltpu.VMEM((chunks, K, CW), BF),
            pltpu.VMEM((chunks, CW, K), BF),
            pltpu.VMEM((chunks, CW, K), BF),
        ] + [pltpu.VMEM((total, NB, NB), F32)] * 3 + [DMA((total,))] * 4,
        compiler_params=pltpu.CompilerParams(
            vmem_limit_bytes=60 << 20, collective_id=0, has_side_effects=True),
        name="merge",
    )(row_values, front_of_row, child_factors, child_columns, damping)[None]


def solution(mesh):
    in_specs = (
        P(("front", "sub"), None),
        P(("front", "sub"), None),
        P("front", "sub", None),
        P("front", None),
        P("front", None),
    )
    out_specs = P("front", "sub", None)
    return jax.shard_map(local, mesh=mesh, in_specs=in_specs, out_specs=out_specs, check_vma=False)
```

```python
import functools
import jax, jax.numpy as jnp
from jax import lax
from jax.experimental import pallas as pl
from jax.experimental.pallas import tpu as pltpu
from jax.sharding import PartitionSpec as P

NB = 128
CW = 2 * NB
BF = jnp.bfloat16
F32 = jnp.float32


def split3(x):
    h = x.astype(BF)
    r = x - h.astype(F32)
    m = r.astype(BF)
    l = (r - m.astype(F32)).astype(BF)
    return h, m, l


def split2(x):
    h = x.astype(BF)
    return h, (x - h.astype(F32)).astype(BF)


def tdot(a, b):
    return lax.dot_general(a, b, (((0,), (0,)), ((), ())), preferred_element_type=F32)


def mm(a, b):
    return lax.dot_general(a, b, (((1,), (0,)), ((), ())), preferred_element_type=F32)


def factor_diag(m_ref, B, slot):
    for b in range(NB // B):
        lo = b * B
        slot(b)
        rows = m_ref[lo:lo + B, :]
        sub = lax.broadcasted_iota(jnp.int32, (B, 1), 0)
        cs = [jnp.broadcast_to(rows[:, lo + j:lo + j + 1], (B, NB)) for j in range(B)]
        for j in range(B):
            c = cs[j]
            r = lax.rsqrt(c[j:j + 1, :])
            mult = jnp.where(sub > j, c * r, 0.0)
            r2 = jnp.concatenate([r, r], axis=1)
            pivot = rows[j:j + 1, :] * r2
            m2 = jnp.concatenate([mult, mult], axis=1)
            rows = jnp.where(sub == j, pivot, rows - m2 * pivot)
            for i in range(j + 1, B):
                cs[i] = cs[i] - mult * (cs[i][j:j + 1, :] * r)
        m_ref[lo:lo + B, :] = rows
        if lo + B < NB:
            h, m, l = split3(rows)
            left = jnp.concatenate([h, h, m, h, l, m], axis=0)[:, :NB]
            right = jnp.concatenate([h, m, h, l, h, m], axis=0)
            upd = tdot(left, right)
            m_ref[lo + B:, :] = m_ref[lo + B:, :] - upd[lo + B:, :]


MESH = pl.DeviceIdType.MESH


def dot3(lhs, h, l):
    return mm(lhs, jnp.concatenate([h, l, h], axis=0))


def left3(h, l):
    return jnp.concatenate([h, h, l], axis=1)


def fused_body(n, fronts, cap, B, x_ref, d_ref, ch_ref, cc_ref, w_ref, o_ref, out_ref, in_ref, fs, fg, a_ref, m_ref, rt_ref, rr_ref, mh_ref, ml_ref, tt_ref, xh_ref, xl_ref, th_ref, tl_ref, p_ref, l_ref, f_ref, dp_ref, dl_ref, df_ref, dr_ref, rd_ref, ss, sg, ds, dg, os, og, ps, pg, go):
    R, F = x_ref.shape
    kids, crows, _ = ch_ref.shape
    slots = fronts * cap
    panels = F // NB
    chunks = F // CW
    me = lax.axis_index("sub")
    mine = lax.axis_index("front")
    side = lax.rem(mine, 2)
    pos = me + side * (n - 1 - 2 * me)
    top = (n - 1) * (1 - side)
    step = 1 - 2 * side
    is_root = pos == n - 1
    is_first = pos == 0

    barrier = pltpu.get_barrier_semaphore()

    def greet_sub(k, c):
        pl.semaphore_signal(barrier, inc=1, device_id={"sub": lax.rem(me + k, n)}, device_id_type=MESH)
        return c

    def greet_front(k, c):
        pl.semaphore_signal(barrier, inc=1, device_id={"front": lax.rem(mine + k, fronts)}, device_id_type=MESH)
        return c

    lax.fori_loop(1, n, greet_sub, 0)
    lax.fori_loop(1, fronts, greet_front, 0)

    def cols_of(c):
        return pl.ds(pl.multiple_of(c * CW, CW), CW)

    def rows_of(f):
        return pl.ds(pl.multiple_of(f * cap, cap), cap)

    def post(k, c, dst_front):
        to = lax.rem(mine + k, fronts)
        return pltpu.make_async_remote_copy(
            src_ref=out_ref.at[c, rows_of(to)], dst_ref=in_ref.at[c, rows_of(dst_front)], send_sem=fs.at[c, k],
            recv_sem=fg.at[c, k], device_id={"front": to}, device_id_type=MESH)

    dest = d_ref[...]
    hot = dest == lax.broadcasted_iota(jnp.int32, (fronts, R), 0)
    above = lax.broadcasted_iota(jnp.int32, (R, R), 0) < lax.broadcasted_iota(jnp.int32, (R, R), 1)
    before = mm(hot.astype(F32).astype(BF), above.astype(F32).astype(BF))
    position = jnp.sum(jnp.where(hot, before, 0.0), axis=0, keepdims=True)
    slot_of = dest.astype(F32) * cap + position
    pick = (slot_of == lax.broadcasted_iota(jnp.int32, (slots, R), 0).astype(F32)).astype(F32).astype(BF)
    pick2 = jnp.concatenate([pick, pick], axis=1)

    def route(c):
        out_ref[c] = mm(pick2, jnp.concatenate(split2(x_ref[:, cols_of(c)]), axis=0))

    def post_rows(c):
        def one(k, cc):
            post(k, c, mine).start()
            return cc

        lax.fori_loop(1, fronts, one, 0)
        in_ref[c, rows_of(mine), :] = out_ref[c, rows_of(mine), :]

    route(0)
    pl.semaphore_wait(barrier, fronts + n - 2)
    post_rows(0)

    def route_rest(c, cc):
        route(c)
        post_rows(c)
        return cc

    lax.fori_loop(1, chunks, route_rest, 0)

    def place_kids(c, cc):
        for kid in range(kids):
            h, l = split2(ch_ref[kid])
            spread = (lax.broadcasted_iota(jnp.int32, (CW, cc_ref.shape[1]), 0) + c * CW == cc_ref[kid:kid + 1, :]).astype(F32).astype(BF)
            both = lax.dot_general(jnp.concatenate([h, l], axis=0), spread, (((1,), (1,)), ((), ())), preferred_element_type=F32)
            xh_ref[c, kid * crows:(kid + 1) * crows, :] = both[:crows].astype(BF)
            xl_ref[c, kid * crows:(kid + 1) * crows, :] = both[crows:].astype(BF)
        return cc

    lax.fori_loop(0, chunks, place_kids, 0)

    ri = lax.broadcasted_iota(jnp.int32, (NB, NB), 0)
    ci = lax.broadcasted_iota(jnp.int32, (NB, NB), 1)

    def place(i, j):
        return j * (j + 1) // 2 + i

    def hop(src, dst, c, send, recv):
        return pltpu.make_async_remote_copy(
            src_ref=src.at[c], dst_ref=dst.at[c], send_sem=send.at[c], recv_sem=recv.at[c],
            device_id={"sub": lax.rem(me + step + n, n)}, device_id_type=MESH)

    def hop_block(src, c):
        return hop(src, l_ref, c, ss, sg)

    def hop_pair(src, J):
        return hop(src, dl_ref, J, ds, dg)

    def stream(copy, own, came, sums, c):
        @pl.when(is_first)
        def _():
            copy(own, c).start()

        @pl.when((pos > 0) & (pos < n - 1))
        def _():
            copy(sums, c).wait_recv()
            sums[c] = came[c] + own[c]
            copy(sums, c).start()

    def pack(ref, c, a, b):
        ref[c, :NB, :] = jnp.where(ci >= ri, a, b)
        ref[c, NB:, :] = jnp.broadcast_to(jnp.sum(jnp.where(ri == ci, b, 0.0), axis=0, keepdims=True), (8, NB))

    def gram_chunk(J, carry):
        def take(k, cc):
            post(k, J, lax.rem(mine + fronts - k, fronts)).wait_recv()
            return cc

        lax.fori_loop(1, fronts, take, 0)
        h, l = split2(in_ref[J])
        xh_ref[J, kids * crows:, :] = h
        xl_ref[J, kids * crows:, :] = l
        th_ref[J] = xh_ref[J].T
        tl_ref[J] = xl_ref[J].T

        def gram_block(I, cc):
            block = dot3(left3(th_ref[I], tl_ref[I]), xh_ref[J], xl_ref[J])
            i, j = 2 * I, 2 * J
            p_ref[place(i, j + 1)] = block[:NB, NB:]

            @pl.when(J > I)
            def _():
                p_ref[place(i, j)] = block[:NB, :NB]
                p_ref[place(i + 1, j)] = block[NB:, :NB]
                p_ref[place(i + 1, j + 1)] = block[NB:, NB:]
                stream(hop_block, p_ref, l_ref, f_ref, place(i, j))
                stream(hop_block, p_ref, l_ref, f_ref, place(i + 1, j))

            @pl.when(J == I)
            def _():
                pack(dp_ref, J, block[:NB, :NB], block[NB:, NB:])
                stream(hop_pair, dp_ref, dl_ref, df_ref, J)

            stream(hop_block, p_ref, l_ref, f_ref, place(i, j + 1))

            @pl.when(J > I)
            def _():
                stream(hop_block, p_ref, l_ref, f_ref, place(i + 1, j + 1))
            return cc

        return lax.fori_loop(0, J + 1, gram_block, carry)

    lax.fori_loop(0, chunks, gram_chunk, 0)

    def at(i, j):
        return (pl.ds(pl.multiple_of(i * NB, NB), NB), pl.ds(pl.multiple_of(j * NB, NB), NB))

    def at2(i, j):
        return (pl.ds(pl.multiple_of(i * CW, CW), CW), pl.ds(pl.multiple_of(j * CW, CW), CW))

    span = chunks // n

    def ship(Q, P):
        owner = Q // span
        return pltpu.make_async_remote_copy(
            src_ref=a_ref.at[at2(Q, P)], dst_ref=o_ref.at[at2(Q - owner * span, P)], send_sem=os.at[Q, P],
            recv_sem=og.at[Q, P], device_id={"sub": owner}, device_id_type=MESH)

    def ship_side(P):
        owner = P // span
        return pltpu.make_async_remote_copy(
            src_ref=a_ref.at[at(2 * P, 2 * P + 1)], dst_ref=o_ref.at[at(2 * (P - owner * span), 2 * P + 1)],
            send_sem=os.at[P, P], recv_sem=og.at[P, P], device_id={"sub": owner}, device_id_type=MESH)

    def ship_pair(P):
        return pltpu.make_async_remote_copy(
            src_ref=dr_ref.at[P], dst_ref=rd_ref.at[P], send_sem=ps.at[P], recv_sem=pg.at[P],
            device_id={"sub": P // span}, device_id_type=MESH)

    hold = chunks // 2

    def send_column(P):
        def one(Q, cc):
            @pl.when(Q // span == me)
            def _():
                o_ref[at2(Q - me * span, P)] = a_ref[at2(Q, P)]

            @pl.when(Q // span != me)
            def _():
                ship(Q, P).start()
            return cc
        lax.fori_loop(0, P, one, 0)

    def send_side(P):
        @pl.when(P // span != me)
        def _():
            ship_side(P).start()

    def send_pair(P):
        @pl.when(P // span != me)
        def _():
            ship_pair(P).start()

    def serve(i, j):
        c = place(i, j)
        hop_block(p_ref, c).wait_recv()
        a_ref[at(i, j)] = p_ref[c] + l_ref[c]

    def serve_pair(P):
        hop_pair(dp_ref, P).wait_recv()
        m = dp_ref[P, :NB, :] + dl_ref[P, :NB, :]
        d = dp_ref[P, NB:, :] + dl_ref[P, NB:, :]
        mt = m.T
        for k, block in ((0, jnp.where(ci >= ri, m, mt)), (1, jnp.where(ci > ri, mt, jnp.where(ci < ri, m, d[:1])))):
            i = 2 * P + k
            wt = w_ref[:, pl.ds(pl.multiple_of(i * NB, NB), NB)]
            a_ref[at(i, i)] = block + jnp.where(ri == ci, wt * wt, 0.0)

    def factor(p):
        m_ref[:, :NB] = a_ref[at(p, p)]
        m_ref[:, NB:] = (ri == ci).astype(F32)
        factor_diag(m_ref, B, lambda b: None)
        a_ref[at(p, p)] = jnp.where(ci >= ri, m_ref[:, :NB], 0.0)
        return jnp.where(ci <= ri, m_ref[:, NB:], 0.0)

    def keep_t(P, r0, c0, t):
        h, l = split2(t)
        tt_ref[P, r0:r0 + NB, c0:c0 + NB] = h
        tt_ref[P, r0:r0 + NB, CW + c0:CW + c0 + NB] = h
        tt_ref[P, r0:r0 + NB, 2 * CW + c0:2 * CW + c0 + NB] = l

    def supercolumn(P, carry):
        def subtract(I, cc):
            def one(Q, c3):
                a_ref[at2(I, P)] -= mm(rt_ref[Q, I], rr_ref[Q])
                return c3
            return lax.fori_loop(0, I, one, cc)

        def solve(I, cc):
            for i in range(2):
                for j in range(2):
                    serve(2 * I + i, 2 * P + j)
            subtract(I, cc)
            h, l = split2(a_ref[at2(I, P)])
            r = dot3(tt_ref[I], h, l)
            a_ref[at2(I, P)] = r
            h, l = split2(r)
            rr_ref[I] = jnp.concatenate([h, l, h], axis=0)
            rt_ref[I, P] = left3(h.T, l.T)
            return cc

        lax.fori_loop(0, P, solve, 0)

        @pl.when(P == hold)
        def _():
            pl.semaphore_wait(go, 1)

            def backlog(K, cc):
                send_column(K)

                @pl.when(K < P)
                def _():
                    send_side(K)
                    send_pair(K)
                return cc
            lax.fori_loop(0, P + 1, backlog, 0)

        @pl.when(P > hold)
        def _():
            send_column(P)

        serve(2 * P, 2 * P + 1)
        serve_pair(P)
        a_ref[at(2 * P + 1, 2 * P)] = jnp.zeros((NB, NB), F32)
        subtract(P, 0)
        p = 2 * P
        t0 = factor(p)
        h, l = split2(a_ref[at(p, p + 1)])
        th, tl = split2(t0)
        r = dot3(left3(th, tl), h, l)
        a_ref[at(p, p + 1)] = r

        @pl.when(P >= hold)
        def _():
            send_side(P)

        h, l = split2(r)
        rl = left3(h.T, l.T)
        a_ref[at(p + 1, p + 1)] -= dot3(rl, h, l)
        keep_t(P, 0, 0, t0)
        keep_t(P, 0, NB, jnp.zeros((NB, NB), F32))
        mh_ref[...], ml_ref[...] = split2(dot3(rl, th, tl))
        t1 = factor(p + 1)
        a_ref[at(p + 1, p)] = jnp.zeros((NB, NB), F32)

        @pl.when(P // span == me)
        def _():
            o_ref[at2(P - me * span, P)] = a_ref[at2(P, P)]

        @pl.when(P // span != me)
        def _():
            pack(dr_ref, P, a_ref[at(p, p)], a_ref[at(p + 1, p + 1)].T)

        @pl.when(P >= hold)
        def _():
            send_pair(P)

        keep_t(P, NB, NB, t1)
        th, tl = split2(t1)
        keep_t(P, NB, 0, -dot3(left3(th, tl), mh_ref[...], ml_ref[...]))
        return carry

    def over_blocks(lo, hi, fn, pair):
        def row(Q, c):
            def one(P, cc):
                fn(Q, P)
                return cc
            pair(Q)
            return lax.fori_loop(Q + 1, chunks, one, c)
        lax.fori_loop(lo, hi, row, 0)

    def blank(i, c):
        def one(j, cc):
            o_ref[at2(i, j)] = jnp.zeros((CW, CW), F32)
            return cc
        return lax.fori_loop(0, me * span + i, one, c)

    lax.fori_loop(0, span, blank, 0)

    @pl.when(is_root)
    def _():
        lax.fori_loop(0, chunks, supercolumn, 0)

        def sent(Q, P):
            @pl.when(Q // span != me)
            def _():
                ship(Q, P).wait_send()

        def sent_pair(P):
            @pl.when(P // span != me)
            def _():
                ship_side(P).wait_send()
                ship_pair(P).wait_send()

        over_blocks(0, chunks, sent, sent_pair)

    @pl.when(jnp.logical_not(is_root))
    def _():
        def sent(c, cc):
            hop_pair(df_ref, c).wait_send()
            hop_block(f_ref, place(2 * c, 2 * c + 1)).wait_send()

            def off(i, c3):
                hop_block(f_ref, place(i, 2 * c)).wait_send()
                hop_block(f_ref, place(i, 2 * c + 1)).wait_send()
                return c3
            return lax.fori_loop(0, 2 * c, off, cc)
        lax.fori_loop(0, chunks, sent, 0)

        @pl.when(is_first)
        def _():
            pl.semaphore_signal(go, inc=1, device_id={"front": mine + 1 - 2 * side}, device_id_type=MESH)

        def came(Q, P):
            ship(Q, P).wait_recv()

        def came_pair(P):
            ship_side(P).wait_recv()
            ship_pair(P).wait_recv()
            k = 2 * (P - me * span)
            m = rd_ref[P, :NB, :]
            o_ref[at(k, 2 * P)] = jnp.where(ci >= ri, m, 0.0)
            o_ref[at(k + 1, 2 * P)] = jnp.zeros((NB, NB), F32)
            o_ref[at(k + 1, 2 * P + 1)] = jnp.where(ci > ri, m.T, jnp.where(ci == ri, rd_ref[P, NB:NB + 1, :], 0.0))

        over_blocks(me * span, me * span + span, came, came_pair)


    def sent_rows(c, cc):
        def one(k, c3):
            post(k, c, mine).wait_send()
            return c3
        return lax.fori_loop(1, fronts, one, cc)

    lax.fori_loop(0, chunks, sent_rows, 0)


def local(row_values, front_of_row, child_factors, child_columns, damping, B=16):
    fronts, n = lax.axis_size("front"), lax.axis_size("sub")
    rows_held, F = row_values.shape
    cap = -(-(2 * rows_held // fronts) // 8) * 8
    K = fronts * cap + child_factors.shape[0] * child_factors.shape[1]
    panels, chunks = F // NB, F // CW
    total = panels * (panels + 1) // 2
    DMA = pltpu.SemaphoreType.DMA
    return pl.pallas_call(
        functools.partial(fused_body, n, fronts, cap, B),
        out_shape=jax.ShapeDtypeStruct((F // n, F), F32),
        in_specs=[pl.BlockSpec(memory_space=pltpu.VMEM)] * 5,
        out_specs=pl.BlockSpec(memory_space=pltpu.VMEM),
        scratch_shapes=[
            pltpu.VMEM((chunks, fronts * cap, CW), F32),
            pltpu.VMEM((chunks, fronts * cap, CW), F32),
            DMA((chunks, fronts)),
            DMA((chunks, fronts)),
            pltpu.VMEM((F, F), F32),
            pltpu.VMEM((NB, 2 * NB), F32),
            pltpu.VMEM((chunks, chunks, CW, 3 * CW), BF),
            pltpu.VMEM((chunks, 3 * CW, CW), BF),
            pltpu.VMEM((NB, NB), BF),
            pltpu.VMEM((NB, NB), BF),
            pltpu.VMEM((chunks, CW, 3 * CW), BF),
            pltpu.VMEM((chunks, K, CW), BF),
            pltpu.VMEM((chunks, K, CW), BF),
            pltpu.VMEM((chunks, CW, K), BF),
            pltpu.VMEM((chunks, CW, K), BF),
        ] + [pltpu.VMEM((total, NB, NB), F32)] * 3 + [pltpu.VMEM((chunks, NB + 8, NB), F32)] * 5
        + [DMA((total,))] * 2 + [DMA((chunks,))] * 2 + [DMA((chunks, chunks))] * 2 + [DMA((chunks,))] * 2 + [pltpu.SemaphoreType.REGULAR],
        compiler_params=pltpu.CompilerParams(
            vmem_limit_bytes=60 << 20, collective_id=0, has_side_effects=True),
        name="merge",
    )(row_values, front_of_row.reshape(1, rows_held), child_factors, child_columns, damping)[None]


def solution(mesh):
    in_specs = (
        P(("front", "sub"), None),
        P(("front", "sub"), None),
        P("front", "sub", None),
        P("front", None),
        P("front", None),
    )
    out_specs = P("front", "sub", None)
    return jax.shard_map(local, mesh=mesh, in_specs=in_specs, out_specs=out_specs, check_vma=False)
```

```python
import functools
import jax, jax.numpy as jnp
from jax import lax
from jax.experimental import pallas as pl
from jax.experimental.pallas import tpu as pltpu
from jax.sharding import PartitionSpec as P

NB = 128
CW = 2 * NB
BF = jnp.bfloat16
F32 = jnp.float32


def split2(x):
    h = x.astype(BF)
    return h, (x - h.astype(F32)).astype(BF)


def mm(a, b):
    return lax.dot_general(a, b, (((1,), (0,)), ((), ())), preferred_element_type=F32)


def wide(x):
    return jnp.concatenate([x, x], axis=1)


def factor_diag(m_ref, B):
    sub = lax.broadcasted_iota(jnp.int32, (8, 1), 0)
    T = B // 8

    def tiles(x):
        return [x[8 * t:8 * t + 8] for t in range(T)]

    def row(x, s):
        return jnp.broadcast_to(x[s:s + 1, :], x.shape)

    def spread(x, j):
        return jnp.broadcast_to(x[:, j:j + 1], (8, NB))

    rows = tiles(m_ref[:B, :])
    for lo in range(0, NB, B):
        cs = [[spread(x, lo + j) for x in rows] for j in range(B)]
        if lo + B < NB:
            nxt = tiles(m_ref[lo + B:lo + 2 * B, :])
            raw = [[spread(x, lo + j) for x in nxt] for j in range(B)]
        done, scale = list(rows), [jnp.zeros((8, NB), F32)] * T
        for j in range(B):
            tj, sj = j // 8, j % 8
            here = sub == sj
            r = lax.rsqrt(row(cs[j][tj], sj))
            half = [(jnp.where(here, 0.0, x) if t == tj else x) * r for t, x in enumerate(cs[j])]
            q = [x * r for x in half]
            done[tj] = jnp.where(here, rows[tj], done[tj])
            scale[tj] = jnp.where(here, r, scale[tj])
            for i in range(j + 1, B):
                u = row(cs[i][tj], sj)
                if i == j + 1:
                    ur = u * r
                    cs[i] = [x - y * ur for x, y in zip(cs[i], half)]
                else:
                    cs[i] = [x - y * u for x, y in zip(cs[i], q)]
            p = row(rows[tj], sj)
            rows = [x - wide(y) * p for x, y in zip(rows, q)]
        m_ref[lo:lo + B, :] = jnp.concatenate([x * wide(y) for x, y in zip(done, scale)], axis=0)
        if lo + B < NB:
            w = [x * wide(y * y) for x, y in zip(rows, scale)]
            if lo + 2 * B < NB:
                rest = m_ref[lo + 2 * B:, :]
                h, l = split2(rest[:, :NB])

                def padded(x):
                    above = [jnp.zeros((lo, 2 * NB), BF)] if lo else []
                    return jnp.concatenate(above + [x, jnp.zeros((NB - lo - B, 2 * NB), BF)], axis=0)

                wh, wl = map(padded, split2(jnp.concatenate(w, axis=0)))
                m_ref[lo + 2 * B:, :] = rest - mm(left3(h, l), jnp.concatenate([wh, wl, wh], axis=0))
            rows = []
            for t in range(T):
                terms = [wide(raw[k][t]) * row(w[k // 8], k % 8) for k in range(B)]
                sums = [sum(terms[g + 2:B:2], terms[g]) for g in range(2)]
                rows.append(nxt[t] - (sums[0] + sums[1]))


MESH = pl.DeviceIdType.MESH


def dot3(lhs, h, l):
    return mm(lhs, jnp.concatenate([h, l, h], axis=0))


def left3(h, l):
    return jnp.concatenate([h, h, l], axis=1)


def fused_body(n, fronts, cap, B, x_ref, d_ref, ch_ref, cc_ref, w_ref, o_ref, out_ref, in_ref, fs, fg, a_ref, m_ref, rt_ref, rr_ref, mh_ref, ml_ref, tt_ref, xh_ref, xl_ref, th_ref, tl_ref, p_ref, l_ref, f_ref, dp_ref, dl_ref, df_ref, dr_ref, rd_ref, ss, sg, ds, dg, os, og, ps, pg, go):
    R, F = x_ref.shape
    kids, crows, _ = ch_ref.shape
    slots = fronts * cap
    panels = F // NB
    chunks = F // CW
    me = lax.axis_index("sub")
    mine = lax.axis_index("front")
    side = lax.rem(mine, 2)
    pos = me + side * (n - 1 - 2 * me)
    top = (n - 1) * (1 - side)
    step = 1 - 2 * side
    is_root = pos == n - 1
    is_first = pos == 0

    barrier = pltpu.get_barrier_semaphore()

    def greet_sub(k, c):
        pl.semaphore_signal(barrier, inc=1, device_id={"sub": lax.rem(me + k, n)}, device_id_type=MESH)
        return c

    def greet_front(k, c):
        pl.semaphore_signal(barrier, inc=1, device_id={"front": lax.rem(mine + k, fronts)}, device_id_type=MESH)
        return c

    lax.fori_loop(1, n, greet_sub, 0)
    lax.fori_loop(1, fronts, greet_front, 0)

    def cols_of(c):
        return pl.ds(pl.multiple_of(c * CW, CW), CW)

    def rows_of(f):
        return pl.ds(pl.multiple_of(f * cap, cap), cap)

    def post(k, c, dst_front):
        to = lax.rem(mine + k, fronts)
        return pltpu.make_async_remote_copy(
            src_ref=out_ref.at[c, rows_of(to)], dst_ref=in_ref.at[c, rows_of(dst_front)], send_sem=fs.at[c, k],
            recv_sem=fg.at[c, k], device_id={"front": to}, device_id_type=MESH)

    dest = d_ref[...]
    hot = dest == lax.broadcasted_iota(jnp.int32, (fronts, R), 0)
    above = lax.broadcasted_iota(jnp.int32, (R, R), 0) < lax.broadcasted_iota(jnp.int32, (R, R), 1)
    before = mm(hot.astype(F32).astype(BF), above.astype(F32).astype(BF))
    position = jnp.sum(jnp.where(hot, before, 0.0), axis=0, keepdims=True)
    slot_of = dest.astype(F32) * cap + position
    pick = (slot_of == lax.broadcasted_iota(jnp.int32, (slots, R), 0).astype(F32)).astype(F32).astype(BF)
    pick2 = jnp.concatenate([pick, pick], axis=1)

    def route(c):
        out_ref[c] = mm(pick2, jnp.concatenate(split2(x_ref[:, cols_of(c)]), axis=0))

    def post_rows(c):
        for odd in (1, 0):
            def one(t, cc):
                k = lax.rem(2 * t + odd - mine + fronts, fronts)

                @pl.when(k > 0)
                def _():
                    post(k, c, mine).start()
                return cc

            lax.fori_loop(0, fronts // 2, one, 0)
        in_ref[c, rows_of(mine), :] = out_ref[c, rows_of(mine), :]

    route(0)
    pl.semaphore_wait(barrier, fronts + n - 2)
    post_rows(0)

    def route_rest(c, cc):
        route(c)
        post_rows(c)
        return cc

    lax.fori_loop(1, chunks, route_rest, 0)

    def place_kids(c, cc):
        for kid in range(kids):
            h, l = split2(ch_ref[kid])
            spread = (lax.broadcasted_iota(jnp.int32, (CW, cc_ref.shape[1]), 0) + c * CW == cc_ref[kid:kid + 1, :]).astype(F32).astype(BF)
            both = lax.dot_general(jnp.concatenate([h, l], axis=0), spread, (((1,), (1,)), ((), ())), preferred_element_type=F32)
            xh_ref[c, kid * crows:(kid + 1) * crows, :] = both[:crows].astype(BF)
            xl_ref[c, kid * crows:(kid + 1) * crows, :] = both[crows:].astype(BF)
        return cc

    lax.fori_loop(0, chunks, place_kids, 0)

    ri = lax.broadcasted_iota(jnp.int32, (NB, NB), 0)
    ci = lax.broadcasted_iota(jnp.int32, (NB, NB), 1)

    def place(i, j):
        return j * (j + 1) // 2 + i

    def hop(src, dst, c, send, recv):
        return pltpu.make_async_remote_copy(
            src_ref=src.at[c], dst_ref=dst.at[c], send_sem=send.at[c], recv_sem=recv.at[c],
            device_id={"sub": lax.rem(me + step + n, n)}, device_id_type=MESH)

    def hop_block(src, c):
        return hop(src, l_ref, c, ss, sg)

    def hop_pair(src, J):
        return hop(src, dl_ref, J, ds, dg)

    def stream(copy, own, came, sums, c):
        @pl.when(is_first)
        def _():
            copy(own, c).start()

        @pl.when((pos > 0) & (pos < n - 1))
        def _():
            copy(sums, c).wait_recv()
            sums[c] = came[c] + own[c]
            copy(sums, c).start()

    def pack(ref, c, a, b):
        ref[c, :NB, :] = jnp.where(ci >= ri, a, b)
        ref[c, NB:, :] = jnp.broadcast_to(jnp.sum(jnp.where(ri == ci, b, 0.0), axis=0, keepdims=True), (8, NB))

    def gram_chunk(J, carry):
        def take(k, cc):
            post(k, J, lax.rem(mine + fronts - k, fronts)).wait_recv()
            return cc

        lax.fori_loop(1, fronts, take, 0)
        h, l = split2(in_ref[J])
        xh_ref[J, kids * crows:, :] = h
        xl_ref[J, kids * crows:, :] = l
        th_ref[J] = xh_ref[J].T
        tl_ref[J] = xl_ref[J].T

        def gram_block(I, cc):
            block = dot3(left3(th_ref[I], tl_ref[I]), xh_ref[J], xl_ref[J])
            i, j = 2 * I, 2 * J
            p_ref[place(i, j + 1)] = block[:NB, NB:]

            @pl.when(J > I)
            def _():
                p_ref[place(i, j)] = block[:NB, :NB]
                p_ref[place(i + 1, j)] = block[NB:, :NB]
                p_ref[place(i + 1, j + 1)] = block[NB:, NB:]
                stream(hop_block, p_ref, l_ref, f_ref, place(i, j))
                stream(hop_block, p_ref, l_ref, f_ref, place(i + 1, j))

            @pl.when(J == I)
            def _():
                pack(dp_ref, J, block[:NB, :NB], block[NB:, NB:])
                stream(hop_pair, dp_ref, dl_ref, df_ref, J)

            stream(hop_block, p_ref, l_ref, f_ref, place(i, j + 1))

            @pl.when(J > I)
            def _():
                stream(hop_block, p_ref, l_ref, f_ref, place(i + 1, j + 1))
            return cc

        return lax.fori_loop(0, J + 1, gram_block, carry)

    lax.fori_loop(0, chunks, gram_chunk, 0)

    def at(i, j):
        return (pl.ds(pl.multiple_of(i * NB, NB), NB), pl.ds(pl.multiple_of(j * NB, NB), NB))

    def at2(i, j):
        return (pl.ds(pl.multiple_of(i * CW, CW), CW), pl.ds(pl.multiple_of(j * CW, CW), CW))

    span = chunks // n

    def ship(Q, P):
        owner = Q // span
        return pltpu.make_async_remote_copy(
            src_ref=a_ref.at[at2(Q, P)], dst_ref=o_ref.at[at2(Q - owner * span, P)], send_sem=os.at[Q, P],
            recv_sem=og.at[Q, P], device_id={"sub": owner}, device_id_type=MESH)

    def ship_side(P):
        owner = P // span
        return pltpu.make_async_remote_copy(
            src_ref=a_ref.at[at(2 * P, 2 * P + 1)], dst_ref=o_ref.at[at(2 * (P - owner * span), 2 * P + 1)],
            send_sem=os.at[P, P], recv_sem=og.at[P, P], device_id={"sub": owner}, device_id_type=MESH)

    def ship_pair(P):
        return pltpu.make_async_remote_copy(
            src_ref=dr_ref.at[P], dst_ref=rd_ref.at[P], send_sem=ps.at[P], recv_sem=pg.at[P],
            device_id={"sub": P // span}, device_id_type=MESH)

    hold = chunks // 2

    def send_block(Q, P):
        @pl.when(Q // span == me)
        def _():
            o_ref[at2(Q - me * span, P)] = a_ref[at2(Q, P)]

        @pl.when(Q // span != me)
        def _():
            ship(Q, P).start()

    def send_column(P):
        def one(Q, cc):
            send_block(Q, P)
            return cc
        lax.fori_loop(0, P, one, 0)

    def send_side(P):
        @pl.when(P // span != me)
        def _():
            ship_side(P).start()

    def send_pair(P):
        @pl.when(P // span != me)
        def _():
            ship_pair(P).start()

    def serve(i, j):
        c = place(i, j)
        hop_block(p_ref, c).wait_recv()
        a_ref[at(i, j)] = p_ref[c] + l_ref[c]

    def serve_pair(P):
        hop_pair(dp_ref, P).wait_recv()
        m = dp_ref[P, :NB, :] + dl_ref[P, :NB, :]
        d = dp_ref[P, NB:, :] + dl_ref[P, NB:, :]
        mt = m.T
        for k, block in ((0, jnp.where(ci >= ri, m, mt)), (1, jnp.where(ci > ri, mt, jnp.where(ci < ri, m, d[:1])))):
            i = 2 * P + k
            wt = w_ref[:, pl.ds(pl.multiple_of(i * NB, NB), NB)]
            a_ref[at(i, i)] = block + jnp.where(ri == ci, wt * wt, 0.0)

    def factor(p):
        m_ref[:, :NB] = a_ref[at(p, p)]
        m_ref[:, NB:] = (ri == ci).astype(F32)
        factor_diag(m_ref, B)
        a_ref[at(p, p)] = jnp.where(ci >= ri, m_ref[:, :NB], 0.0)
        return jnp.where(ci <= ri, m_ref[:, NB:], 0.0)

    def keep_t(P, r0, c0, t):
        h, l = split2(t)
        tt_ref[P, r0:r0 + NB, c0:c0 + NB] = h
        tt_ref[P, r0:r0 + NB, CW + c0:CW + c0 + NB] = h
        tt_ref[P, r0:r0 + NB, 2 * CW + c0:2 * CW + c0 + NB] = l

    def supercolumn(P, carry):
        def subtract(I, cc):
            def one(Q, c3):
                a_ref[at2(I, P)] -= mm(rt_ref[Q, I], rr_ref[Q])
                return c3
            return lax.fori_loop(0, I, one, cc)

        def solve(I, cc):
            for i in range(2):
                for j in range(2):
                    serve(2 * I + i, 2 * P + j)
            subtract(I, cc)
            h, l = split2(a_ref[at2(I, P)])
            r = dot3(tt_ref[I], h, l)
            a_ref[at2(I, P)] = r
            h, l = split2(r)
            rr_ref[I] = jnp.concatenate([h, l, h], axis=0)
            rt_ref[I, P] = left3(h.T, l.T)
            return cc

        lax.fori_loop(0, P, solve, 0)

        @pl.when(P == hold)
        def _():
            pl.semaphore_wait(go, 1)

            def backlog(t, cc):
                Q = side * t + (1 - side) * (P - 1 - t)
                send_side(Q)
                send_pair(Q)

                def one(K, c3):
                    send_block(Q, K)
                    return c3
                return lax.fori_loop(Q + 1, P + 1, one, cc)
            lax.fori_loop(0, P, backlog, 0)

        @pl.when(P > hold)
        def _():
            send_column(P)

        serve(2 * P, 2 * P + 1)
        serve_pair(P)
        a_ref[at(2 * P + 1, 2 * P)] = jnp.zeros((NB, NB), F32)
        subtract(P, 0)
        p = 2 * P
        t0 = factor(p)
        h, l = split2(a_ref[at(p, p + 1)])
        th, tl = split2(t0)
        r = dot3(left3(th, tl), h, l)
        a_ref[at(p, p + 1)] = r

        @pl.when(P >= hold)
        def _():
            send_side(P)

        h, l = split2(r)
        rl = left3(h.T, l.T)
        a_ref[at(p + 1, p + 1)] -= dot3(rl, h, l)
        keep_t(P, 0, 0, t0)
        keep_t(P, 0, NB, jnp.zeros((NB, NB), F32))
        mh_ref[...], ml_ref[...] = split2(dot3(rl, th, tl))
        t1 = factor(p + 1)

        @pl.when(P // span == me)
        def _():
            o_ref[at2(P - me * span, P)] = a_ref[at2(P, P)]

        @pl.when(P // span != me)
        def _():
            pack(dr_ref, P, a_ref[at(p, p)], a_ref[at(p + 1, p + 1)].T)

        @pl.when(P >= hold)
        def _():
            send_pair(P)

        keep_t(P, NB, NB, t1)
        th, tl = split2(t1)
        keep_t(P, NB, 0, -dot3(left3(th, tl), mh_ref[...], ml_ref[...]))
        return carry

    def over_blocks(lo, hi, fn, pair):
        def row(Q, c):
            def one(P, cc):
                fn(Q, P)
                return cc
            pair(Q)
            return lax.fori_loop(Q + 1, chunks, one, c)
        lax.fori_loop(lo, hi, row, 0)

    @pl.when(is_root)
    def _():
        lax.fori_loop(0, chunks, supercolumn, 0)

        def sent(Q, P):
            @pl.when(Q // span != me)
            def _():
                ship(Q, P).wait_send()

        def sent_pair(P):
            @pl.when(P // span != me)
            def _():
                ship_side(P).wait_send()
                ship_pair(P).wait_send()

        over_blocks(0, chunks, sent, sent_pair)

    @pl.when(jnp.logical_not(is_root))
    def _():
        def sent(c, cc):
            hop_pair(df_ref, c).wait_send()
            hop_block(f_ref, place(2 * c, 2 * c + 1)).wait_send()

            def off(i, c3):
                hop_block(f_ref, place(i, 2 * c)).wait_send()
                hop_block(f_ref, place(i, 2 * c + 1)).wait_send()
                return c3
            return lax.fori_loop(0, 2 * c, off, cc)
        lax.fori_loop(0, chunks, sent, 0)

        @pl.when(is_first)
        def _():
            pl.semaphore_signal(go, inc=1, device_id={"front": mine + 1 - 2 * side}, device_id_type=MESH)

        def came(Q, P):
            ship(Q, P).wait_recv()

        def came_pair(P):
            ship_side(P).wait_recv()
            ship_pair(P).wait_recv()
            k = 2 * (P - me * span)
            m = rd_ref[P, :NB, :]
            o_ref[at(k, 2 * P)] = jnp.where(ci >= ri, m, 0.0)
            o_ref[at(k + 1, 2 * P + 1)] = jnp.where(ci > ri, m.T, jnp.where(ci == ri, rd_ref[P, NB:NB + 1, :], 0.0))

        over_blocks(me * span, me * span + span, came, came_pair)


    def sent_rows(c, cc):
        def one(k, c3):
            post(k, c, mine).wait_send()
            return c3
        return lax.fori_loop(1, fronts, one, cc)

    lax.fori_loop(0, chunks, sent_rows, 0)


def local(row_values, front_of_row, child_factors, child_columns, damping, B=16):
    fronts, n = lax.axis_size("front"), lax.axis_size("sub")
    rows_held, F = row_values.shape
    cap = -(-(2 * rows_held // fronts) // 8) * 8
    K = fronts * cap + child_factors.shape[0] * child_factors.shape[1]
    panels, chunks = F // NB, F // CW
    total = panels * (panels + 1) // 2
    DMA = pltpu.SemaphoreType.DMA
    out = pl.pallas_call(
        functools.partial(fused_body, n, fronts, cap, B),
        out_shape=jax.ShapeDtypeStruct((F // n, F), F32),
        in_specs=[pl.BlockSpec(memory_space=pltpu.VMEM)] * 5,
        out_specs=pl.BlockSpec(memory_space=pltpu.VMEM),
        scratch_shapes=[
            pltpu.VMEM((chunks, fronts * cap, CW), F32),
            pltpu.VMEM((chunks, fronts * cap, CW), F32),
            DMA((chunks, fronts)),
            DMA((chunks, fronts)),
            pltpu.VMEM((F, F), F32),
            pltpu.VMEM((NB, 2 * NB), F32),
            pltpu.VMEM((chunks, chunks, CW, 3 * CW), BF),
            pltpu.VMEM((chunks, 3 * CW, CW), BF),
            pltpu.VMEM((NB, NB), BF),
            pltpu.VMEM((NB, NB), BF),
            pltpu.VMEM((chunks, CW, 3 * CW), BF),
            pltpu.VMEM((chunks, K, CW), BF),
            pltpu.VMEM((chunks, K, CW), BF),
            pltpu.VMEM((chunks, CW, K), BF),
            pltpu.VMEM((chunks, CW, K), BF),
        ] + [pltpu.VMEM((total, NB, NB), F32)] * 3 + [pltpu.VMEM((chunks, NB + 8, NB), F32)] * 5
        + [DMA((total,))] * 2 + [DMA((chunks,))] * 2 + [DMA((chunks, chunks))] * 2 + [DMA((chunks,))] * 2 + [pltpu.SemaphoreType.REGULAR],
        compiler_params=pltpu.CompilerParams(
            vmem_limit_bytes=(26 << 20) + 8 * (K + fronts * cap) * F, collective_id=0, has_side_effects=True),
        name="merge",
    )(row_values, front_of_row.reshape(1, rows_held), child_factors, child_columns, damping)
    held = F // n
    below = lax.axis_index("sub") * held + lax.broadcasted_iota(jnp.int32, (held, F), 0) > lax.broadcasted_iota(jnp.int32, (held, F), 1)
    return jnp.where(below, 0.0, out)[None]


def solution(mesh):
    in_specs = (
        P(("front", "sub"), None),
        P(("front", "sub"), None),
        P("front", "sub", None),
        P("front", None),
        P("front", None),
    )
    out_specs = P("front", "sub", None)
    return jax.shard_map(local, mesh=mesh, in_specs=in_specs, out_specs=out_specs, check_vma=False)
```

```python
import functools
import jax, jax.numpy as jnp
from jax import lax
from jax.experimental import pallas as pl
from jax.experimental.pallas import tpu as pltpu
from jax.sharding import PartitionSpec as P

NB = 128
CW = 2 * NB
BF = jnp.bfloat16
F32 = jnp.float32


def split2(x):
    h = x.astype(BF)
    return h, (x - h.astype(F32)).astype(BF)


def mm(a, b):
    return lax.dot_general(a, b, (((1,), (0,)), ((), ())), preferred_element_type=F32)


def wide(x):
    return jnp.concatenate([x, x], axis=1)


def factor_diag(m_ref, B):
    sub = lax.broadcasted_iota(jnp.int32, (8, 1), 0)
    T = B // 8

    def tiles(x):
        return [x[8 * t:8 * t + 8] for t in range(T)]

    def row(x, s):
        return jnp.broadcast_to(x[s:s + 1, :], x.shape)

    def spread(x, j):
        return jnp.broadcast_to(x[:, j:j + 1], (8, NB))

    rows = tiles(m_ref[:B, :])
    for lo in range(0, NB, B):
        cs = [[spread(x, lo + j) for x in rows] for j in range(B)]
        if lo + B < NB:
            nxt = tiles(m_ref[lo + B:lo + 2 * B, :])
            raw = [[spread(x, lo + j) for x in nxt] for j in range(B)]
        done, scale = list(rows), [jnp.zeros((8, NB), F32)] * T
        for j in range(B):
            tj, sj = j // 8, j % 8
            here = sub == sj
            r = lax.rsqrt(row(cs[j][tj], sj))
            half = [(jnp.where(here, 0.0, x) if t == tj else x) * r for t, x in enumerate(cs[j])]
            q = [x * r for x in half]
            done[tj] = jnp.where(here, rows[tj], done[tj])
            scale[tj] = jnp.where(here, r, scale[tj])
            for i in range(j + 1, B):
                u = row(cs[i][tj], sj)
                if i == j + 1:
                    ur = u * r
                    cs[i] = [x - y * ur for x, y in zip(cs[i], half)]
                else:
                    cs[i] = [x - y * u for x, y in zip(cs[i], q)]
            p = row(rows[tj], sj)
            rows = [x - wide(y) * p for x, y in zip(rows, q)]
        m_ref[lo:lo + B, :] = jnp.concatenate([x * wide(y) for x, y in zip(done, scale)], axis=0)
        if lo + B < NB:
            w = [x * wide(y * y) for x, y in zip(rows, scale)]
            if lo + 2 * B < NB:
                rest = m_ref[lo + 2 * B:, :]
                h, l = split2(rest[:, :NB])

                def padded(x):
                    above = [jnp.zeros((lo, 2 * NB), BF)] if lo else []
                    return jnp.concatenate(above + [x, jnp.zeros((NB - lo - B, 2 * NB), BF)], axis=0)

                wh, wl = map(padded, split2(jnp.concatenate(w, axis=0)))
                m_ref[lo + 2 * B:, :] = rest - mm(left3(h, l), jnp.concatenate([wh, wl, wh], axis=0))
            rows = []
            for t in range(T):
                terms = [wide(raw[k][t]) * row(w[k // 8], k % 8) for k in range(B)]
                sums = [sum(terms[g + 2:B:2], terms[g]) for g in range(2)]
                rows.append(nxt[t] - (sums[0] + sums[1]))


MESH = pl.DeviceIdType.MESH


def dot3(lhs, h, l):
    return mm(lhs, jnp.concatenate([h, l, h], axis=0))


def left3(h, l):
    return jnp.concatenate([h, h, l], axis=1)


def fused_body(n, fronts, cap, B, x_hbm, d_hbm, ch_hbm, cc_hbm, w_hbm, o_ref, x_ref, d_ref, ch_ref, cc_ref, w_ref, ls, out_ref, in_ref, fs, fg, a_ref, m_ref, rt_ref, rr_ref, mh_ref, ml_ref, tt_ref, xh_ref, xl_ref, th_ref, tl_ref, p_ref, l_ref, f_ref, dp_ref, dl_ref, df_ref, dr_ref, rd_ref, ss, sg, ds, dg, os, og, ps, pg, go):
    R, F = x_hbm.shape
    kids, crows, _ = ch_hbm.shape
    slots = fronts * cap
    panels = F // NB
    chunks = F // CW
    me = lax.axis_index("sub")
    mine = lax.axis_index("front")
    side = lax.rem(mine, 2)
    pos = me + side * (n - 1 - 2 * me)
    top = (n - 1) * (1 - side)
    step = 1 - 2 * side
    is_root = pos == n - 1
    is_first = pos == 0

    barrier = pltpu.get_barrier_semaphore()

    def greet_sub(k, c):
        pl.semaphore_signal(barrier, inc=1, device_id={"sub": lax.rem(me + k, n)}, device_id_type=MESH)
        return c

    def greet_front(k, c):
        pl.semaphore_signal(barrier, inc=1, device_id={"front": lax.rem(mine + k, fronts)}, device_id_type=MESH)
        return c

    lax.fori_loop(1, n, greet_sub, 0)
    lax.fori_loop(1, fronts, greet_front, 0)

    def cols_of(c):
        return pl.ds(pl.multiple_of(c * CW, CW), CW)

    def rows_of(f):
        return pl.ds(pl.multiple_of(f * cap, cap), cap)

    def post(k, c, dst_front):
        to = lax.rem(mine + k, fronts)
        return pltpu.make_async_remote_copy(
            src_ref=out_ref.at[c, rows_of(to)], dst_ref=in_ref.at[c, rows_of(dst_front)], send_sem=fs.at[c, k],
            recv_sem=fg.at[c, k], device_id={"front": to}, device_id_type=MESH)

    def load(c):
        return pltpu.make_async_copy(x_hbm.at[:, cols_of(c)], x_ref.at[c], ls.at[c])

    small = [pltpu.make_async_copy(src, dst, ls.at[chunks + i]) for i, (src, dst) in enumerate(
        ((d_hbm, d_ref), (ch_hbm, ch_ref), (cc_hbm, cc_ref), (w_hbm, w_ref)))]
    small[0].start()

    def load_all(c, cc):
        load(c).start()
        return cc

    lax.fori_loop(0, chunks, load_all, 0)
    for copy in small[1:]:
        copy.start()
    small[0].wait()
    dest = d_ref[...]
    hot = dest == lax.broadcasted_iota(jnp.int32, (fronts, R), 0)
    above = lax.broadcasted_iota(jnp.int32, (R, R), 0) < lax.broadcasted_iota(jnp.int32, (R, R), 1)
    before = mm(hot.astype(F32).astype(BF), above.astype(F32).astype(BF))
    position = jnp.sum(jnp.where(hot, before, 0.0), axis=0, keepdims=True)
    slot_of = dest.astype(F32) * cap + position
    pick = (slot_of == lax.broadcasted_iota(jnp.int32, (slots, R), 0).astype(F32)).astype(F32).astype(BF)
    pick2 = jnp.concatenate([pick, pick], axis=1)

    def route(c):
        load(c).wait()
        out_ref[c] = mm(pick2, jnp.concatenate(split2(x_ref[c]), axis=0))

    def post_rows(c):
        for odd in (1, 0):
            def one(t, cc):
                k = lax.rem(2 * t + odd - mine + fronts, fronts)

                @pl.when(k > 0)
                def _():
                    post(k, c, mine).start()
                return cc

            lax.fori_loop(0, fronts // 2, one, 0)
        in_ref[c, rows_of(mine), :] = out_ref[c, rows_of(mine), :]

    route(0)
    pl.semaphore_wait(barrier, fronts + n - 2)
    post_rows(0)

    def route_rest(c, cc):
        route(c)
        post_rows(c)
        return cc

    lax.fori_loop(1, chunks, route_rest, 0)

    for copy in small[1:]:
        copy.wait()

    def place_kids(c, cc):
        for kid in range(kids):
            h, l = split2(ch_ref[kid])
            spread = (lax.broadcasted_iota(jnp.int32, (CW, cc_ref.shape[1]), 0) + c * CW == cc_ref[kid:kid + 1, :]).astype(F32).astype(BF)
            both = lax.dot_general(jnp.concatenate([h, l], axis=0), spread, (((1,), (1,)), ((), ())), preferred_element_type=F32)
            xh_ref[c, kid * crows:(kid + 1) * crows, :] = both[:crows].astype(BF)
            xl_ref[c, kid * crows:(kid + 1) * crows, :] = both[crows:].astype(BF)
        return cc

    lax.fori_loop(0, chunks, place_kids, 0)

    ri = lax.broadcasted_iota(jnp.int32, (NB, NB), 0)
    ci = lax.broadcasted_iota(jnp.int32, (NB, NB), 1)

    def place(i, j):
        return j * (j + 1) // 2 + i

    def hop(src, dst, c, send, recv):
        return pltpu.make_async_remote_copy(
            src_ref=src.at[c], dst_ref=dst.at[c], send_sem=send.at[c], recv_sem=recv.at[c],
            device_id={"sub": lax.rem(me + step + n, n)}, device_id_type=MESH)

    def hop_block(src, c):
        return hop(src, l_ref, c, ss, sg)

    def hop_pair(src, J):
        return hop(src, dl_ref, J, ds, dg)

    def stream(copy, own, came, sums, c):
        @pl.when(is_first)
        def _():
            copy(own, c).start()

        @pl.when((pos > 0) & (pos < n - 1))
        def _():
            copy(sums, c).wait_recv()
            sums[c] = came[c] + own[c]
            copy(sums, c).start()

    def pack(ref, c, a, b):
        ref[c, :NB, :] = jnp.where(ci >= ri, a, b)
        ref[c, NB:, :] = jnp.broadcast_to(jnp.sum(jnp.where(ri == ci, b, 0.0), axis=0, keepdims=True), (8, NB))

    def gram_chunk(J, carry):
        def take(k, cc):
            post(k, J, lax.rem(mine + fronts - k, fronts)).wait_recv()
            return cc

        lax.fori_loop(1, fronts, take, 0)
        h, l = split2(in_ref[J])
        xh_ref[J, kids * crows:, :] = h
        xl_ref[J, kids * crows:, :] = l
        th_ref[J] = xh_ref[J].T
        tl_ref[J] = xl_ref[J].T

        def gram_block(I, cc):
            block = dot3(left3(th_ref[I], tl_ref[I]), xh_ref[J], xl_ref[J])
            i, j = 2 * I, 2 * J
            p_ref[place(i, j + 1)] = block[:NB, NB:]

            @pl.when(J > I)
            def _():
                p_ref[place(i, j)] = block[:NB, :NB]
                p_ref[place(i + 1, j)] = block[NB:, :NB]
                p_ref[place(i + 1, j + 1)] = block[NB:, NB:]
                stream(hop_block, p_ref, l_ref, f_ref, place(i, j))
                stream(hop_block, p_ref, l_ref, f_ref, place(i + 1, j))

            @pl.when(J == I)
            def _():
                pack(dp_ref, J, block[:NB, :NB], block[NB:, NB:])
                stream(hop_pair, dp_ref, dl_ref, df_ref, J)

            stream(hop_block, p_ref, l_ref, f_ref, place(i, j + 1))

            @pl.when(J > I)
            def _():
                stream(hop_block, p_ref, l_ref, f_ref, place(i + 1, j + 1))
            return cc

        return lax.fori_loop(0, J + 1, gram_block, carry)

    lax.fori_loop(0, chunks, gram_chunk, 0)

    def at(i, j):
        return (pl.ds(pl.multiple_of(i * NB, NB), NB), pl.ds(pl.multiple_of(j * NB, NB), NB))

    def at2(i, j):
        return (pl.ds(pl.multiple_of(i * CW, CW), CW), pl.ds(pl.multiple_of(j * CW, CW), CW))

    span = chunks // n

    def ship(Q, P):
        owner = Q // span
        return pltpu.make_async_remote_copy(
            src_ref=a_ref.at[at2(Q, P)], dst_ref=o_ref.at[at2(Q - owner * span, P)], send_sem=os.at[Q, P],
            recv_sem=og.at[Q, P], device_id={"sub": owner}, device_id_type=MESH)

    def ship_side(P):
        owner = P // span
        return pltpu.make_async_remote_copy(
            src_ref=a_ref.at[at(2 * P, 2 * P + 1)], dst_ref=o_ref.at[at(2 * (P - owner * span), 2 * P + 1)],
            send_sem=os.at[P, P], recv_sem=og.at[P, P], device_id={"sub": owner}, device_id_type=MESH)

    def ship_pair(P):
        return pltpu.make_async_remote_copy(
            src_ref=dr_ref.at[P], dst_ref=rd_ref.at[P], send_sem=ps.at[P], recv_sem=pg.at[P],
            device_id={"sub": P // span}, device_id_type=MESH)

    hold = chunks // 2

    def send_block(Q, P):
        @pl.when(Q // span == me)
        def _():
            o_ref[at2(Q - me * span, P)] = a_ref[at2(Q, P)]

        @pl.when(Q // span != me)
        def _():
            ship(Q, P).start()

    def send_column(P):
        def one(Q, cc):
            send_block(Q, P)
            return cc
        lax.fori_loop(0, P, one, 0)

    def send_side(P):
        @pl.when(P // span != me)
        def _():
            ship_side(P).start()

    def send_pair(P):
        @pl.when(P // span != me)
        def _():
            ship_pair(P).start()

    def serve(i, j):
        c = place(i, j)
        hop_block(p_ref, c).wait_recv()
        a_ref[at(i, j)] = p_ref[c] + l_ref[c]

    def serve_pair(P):
        hop_pair(dp_ref, P).wait_recv()
        m = dp_ref[P, :NB, :] + dl_ref[P, :NB, :]
        d = dp_ref[P, NB:, :] + dl_ref[P, NB:, :]
        mt = m.T
        for k, block in ((0, jnp.where(ci >= ri, m, mt)), (1, jnp.where(ci > ri, mt, jnp.where(ci < ri, m, d[:1])))):
            i = 2 * P + k
            wt = w_ref[:, pl.ds(pl.multiple_of(i * NB, NB), NB)]
            a_ref[at(i, i)] = block + jnp.where(ri == ci, wt * wt, 0.0)

    def factor(p):
        m_ref[:, :NB] = a_ref[at(p, p)]
        m_ref[:, NB:] = (ri == ci).astype(F32)
        factor_diag(m_ref, B)
        a_ref[at(p, p)] = jnp.where(ci >= ri, m_ref[:, :NB], 0.0)
        return jnp.where(ci <= ri, m_ref[:, NB:], 0.0)

    def keep_t(P, r0, c0, t):
        h, l = split2(t)
        tt_ref[P, r0:r0 + NB, c0:c0 + NB] = h
        tt_ref[P, r0:r0 + NB, CW + c0:CW + c0 + NB] = h
        tt_ref[P, r0:r0 + NB, 2 * CW + c0:2 * CW + c0 + NB] = l

    def supercolumn(P, carry):
        def subtract(I, cc):
            def one(Q, c3):
                a_ref[at2(I, P)] -= mm(rt_ref[Q, I], rr_ref[Q])
                return c3
            return lax.fori_loop(0, I, one, cc)

        def solve(I, cc):
            for i in range(2):
                for j in range(2):
                    serve(2 * I + i, 2 * P + j)
            subtract(I, cc)
            h, l = split2(a_ref[at2(I, P)])
            r = dot3(tt_ref[I], h, l)
            a_ref[at2(I, P)] = r
            h, l = split2(r)
            rr_ref[I] = jnp.concatenate([h, l, h], axis=0)
            rt_ref[I, P] = left3(h.T, l.T)
            return cc

        lax.fori_loop(0, P, solve, 0)

        @pl.when(P == hold)
        def _():
            pl.semaphore_wait(go, 1)

            def backlog(t, cc):
                Q = side * t + (1 - side) * (P - 1 - t)
                send_side(Q)
                send_pair(Q)

                def one(K, c3):
                    send_block(Q, K)
                    return c3
                return lax.fori_loop(Q + 1, P + 1, one, cc)
            lax.fori_loop(0, P, backlog, 0)

        @pl.when(P > hold)
        def _():
            send_column(P)

        serve(2 * P, 2 * P + 1)
        serve_pair(P)
        a_ref[at(2 * P + 1, 2 * P)] = jnp.zeros((NB, NB), F32)
        subtract(P, 0)
        p = 2 * P
        t0 = factor(p)
        h, l = split2(a_ref[at(p, p + 1)])
        th, tl = split2(t0)
        r = dot3(left3(th, tl), h, l)
        a_ref[at(p, p + 1)] = r

        @pl.when(P >= hold)
        def _():
            send_side(P)

        h, l = split2(r)
        rl = left3(h.T, l.T)
        a_ref[at(p + 1, p + 1)] -= dot3(rl, h, l)
        keep_t(P, 0, 0, t0)
        keep_t(P, 0, NB, jnp.zeros((NB, NB), F32))
        mh_ref[...], ml_ref[...] = split2(dot3(rl, th, tl))
        t1 = factor(p + 1)

        @pl.when(P // span == me)
        def _():
            o_ref[at2(P - me * span, P)] = a_ref[at2(P, P)]

        @pl.when(P // span != me)
        def _():
            pack(dr_ref, P, a_ref[at(p, p)], a_ref[at(p + 1, p + 1)].T)

        @pl.when(P >= hold)
        def _():
            send_pair(P)

        keep_t(P, NB, NB, t1)
        th, tl = split2(t1)
        keep_t(P, NB, 0, -dot3(left3(th, tl), mh_ref[...], ml_ref[...]))
        return carry

    def over_blocks(lo, hi, fn, pair):
        def row(Q, c):
            def one(P, cc):
                fn(Q, P)
                return cc
            pair(Q)
            return lax.fori_loop(Q + 1, chunks, one, c)
        lax.fori_loop(lo, hi, row, 0)

    @pl.when(is_root)
    def _():
        lax.fori_loop(0, chunks, supercolumn, 0)

        def sent(Q, P):
            @pl.when(Q // span != me)
            def _():
                ship(Q, P).wait_send()

        def sent_pair(P):
            @pl.when(P // span != me)
            def _():
                ship_side(P).wait_send()
                ship_pair(P).wait_send()

        over_blocks(0, chunks, sent, sent_pair)

    @pl.when(jnp.logical_not(is_root))
    def _():
        def sent(c, lo, hi):
            def off(i, c3):
                hop_block(f_ref, place(i, 2 * c)).wait_send()
                hop_block(f_ref, place(i, 2 * c + 1)).wait_send()
                return c3
            lax.fori_loop(lo, hi, off, 0)

        def sent_diag(c):
            hop_pair(df_ref, c).wait_send()
            hop_block(f_ref, place(2 * c, 2 * c + 1)).wait_send()

        def whole(c, cc):
            sent(c, 0, 2 * c)
            sent_diag(c)
            return cc

        lax.fori_loop(0, chunks - 1, whole, 0)
        sent(chunks - 1, 0, panels - 2 - 0)

        @pl.when(is_first)
        def _():
            pl.semaphore_signal(go, inc=1, device_id={"front": mine + 1 - 2 * side}, device_id_type=MESH)

        sent(chunks - 1, panels - 2 - 0, panels - 2)
        sent_diag(chunks - 1)

        def came(Q, P):
            ship(Q, P).wait_recv()

        def came_pair(P):
            ship_side(P).wait_recv()
            ship_pair(P).wait_recv()
            k = 2 * (P - me * span)
            m = rd_ref[P, :NB, :]
            o_ref[at(k, 2 * P)] = jnp.where(ci >= ri, m, 0.0)
            o_ref[at(k + 1, 2 * P + 1)] = jnp.where(ci > ri, m.T, jnp.where(ci == ri, rd_ref[P, NB:NB + 1, :], 0.0))

        over_blocks(me * span, me * span + span, came, came_pair)


    def sent_rows(c, cc):
        def one(k, c3):
            post(k, c, mine).wait_send()
            return c3
        return lax.fori_loop(1, fronts, one, cc)

    lax.fori_loop(0, chunks, sent_rows, 0)


def local(row_values, front_of_row, child_factors, child_columns, damping, B=16):
    fronts, n = lax.axis_size("front"), lax.axis_size("sub")
    rows_held, F = row_values.shape
    cap = -(-(2 * rows_held // fronts) // 8) * 8
    K = fronts * cap + child_factors.shape[0] * child_factors.shape[1]
    panels, chunks = F // NB, F // CW
    total = panels * (panels + 1) // 2
    DMA = pltpu.SemaphoreType.DMA
    out = pl.pallas_call(
        functools.partial(fused_body, n, fronts, cap, B),
        out_shape=jax.ShapeDtypeStruct((F // n, F), F32),
        in_specs=[pl.BlockSpec(memory_space=pltpu.HBM)] * 5,
        out_specs=pl.BlockSpec(memory_space=pltpu.VMEM),
        scratch_shapes=[
            pltpu.VMEM((chunks, rows_held, CW), F32),
            pltpu.VMEM((1, rows_held), jnp.int32),
            pltpu.VMEM(child_factors.shape, F32),
            pltpu.VMEM(child_columns.shape, jnp.int32),
            pltpu.VMEM(damping.shape, F32),
            DMA((chunks + 4,)),
            pltpu.VMEM((chunks, fronts * cap, CW), F32),
            pltpu.VMEM((chunks, fronts * cap, CW), F32),
            DMA((chunks, fronts)),
            DMA((chunks, fronts)),
            pltpu.VMEM((F, F), F32),
            pltpu.VMEM((NB, 2 * NB), F32),
            pltpu.VMEM((chunks, chunks, CW, 3 * CW), BF),
            pltpu.VMEM((chunks, 3 * CW, CW), BF),
            pltpu.VMEM((NB, NB), BF),
            pltpu.VMEM((NB, NB), BF),
            pltpu.VMEM((chunks, CW, 3 * CW), BF),
            pltpu.VMEM((chunks, K, CW), BF),
            pltpu.VMEM((chunks, K, CW), BF),
            pltpu.VMEM((chunks, CW, K), BF),
            pltpu.VMEM((chunks, CW, K), BF),
        ] + [pltpu.VMEM((total, NB, NB), F32)] * 3 + [pltpu.VMEM((chunks, NB + 8, NB), F32)] * 5
        + [DMA((total,))] * 2 + [DMA((chunks,))] * 2 + [DMA((chunks, chunks))] * 2 + [DMA((chunks,))] * 2 + [pltpu.SemaphoreType.REGULAR],
        compiler_params=pltpu.CompilerParams(
            vmem_limit_bytes=60 << 20, collective_id=0, has_side_effects=True),
        name="merge",
    )(row_values, front_of_row.reshape(1, rows_held), child_factors, child_columns, damping)
    held = F // n
    below = lax.axis_index("sub") * held + lax.broadcasted_iota(jnp.int32, (held, F), 0) > lax.broadcasted_iota(jnp.int32, (held, F), 1)
    return jnp.where(below, 0.0, out)[None]


def solution(mesh):
    in_specs = (
        P(("front", "sub"), None),
        P(("front", "sub"), None),
        P("front", "sub", None),
        P("front", None),
        P("front", None),
    )
    out_specs = P("front", "sub", None)
    return jax.shard_map(local, mesh=mesh, in_specs=in_specs, out_specs=out_specs, check_vma=False)
```

```python
import functools
import jax, jax.numpy as jnp
from jax import lax
from jax.experimental import pallas as pl
from jax.experimental.pallas import tpu as pltpu
from jax.sharding import PartitionSpec as P

NB = 128
CW = 2 * NB
BF = jnp.bfloat16
F32 = jnp.float32


def split2(x):
    h = x.astype(BF)
    return h, (x - h.astype(F32)).astype(BF)


def mm(a, b):
    return lax.dot_general(a, b, (((1,), (0,)), ((), ())), preferred_element_type=F32)


def wide(x):
    return jnp.concatenate([x, x], axis=1)


def factor_diag(m_ref, B):
    sub = lax.broadcasted_iota(jnp.int32, (8, 1), 0)
    T = B // 8

    def tiles(x):
        return [x[8 * t:8 * t + 8] for t in range(T)]

    def row(x, s):
        return jnp.broadcast_to(x[s:s + 1, :], x.shape)

    def spread(x, j):
        return jnp.broadcast_to(x[:, j:j + 1], (8, NB))

    rows = tiles(m_ref[:B, :])
    for lo in range(0, NB, B):
        cs = [[spread(x, lo + j) for x in rows] for j in range(B)]
        if lo + B < NB:
            nxt = tiles(m_ref[lo + B:lo + 2 * B, :])
            raw = [[spread(x, lo + j) for x in nxt] for j in range(B)]
        done, scale = list(rows), [jnp.zeros((8, NB), F32)] * T
        for j in range(B):
            tj, sj = j // 8, j % 8
            here = sub == sj
            r = lax.rsqrt(row(cs[j][tj], sj))
            half = [(jnp.where(here, 0.0, x) if t == tj else x) * r for t, x in enumerate(cs[j])]
            q = [x * r for x in half]
            done[tj] = jnp.where(here, rows[tj], done[tj])
            scale[tj] = jnp.where(here, r, scale[tj])
            for i in range(j + 1, B):
                u = row(cs[i][tj], sj)
                if i == j + 1:
                    ur = u * r
                    cs[i] = [x - y * ur for x, y in zip(cs[i], half)]
                else:
                    cs[i] = [x - y * u for x, y in zip(cs[i], q)]
            p = row(rows[tj], sj)
            rows = [x - wide(y) * p for x, y in zip(rows, q)]
        m_ref[lo:lo + B, :] = jnp.concatenate([x * wide(y) for x, y in zip(done, scale)], axis=0)
        if lo + B < NB:
            w = [x * wide(y * y) for x, y in zip(rows, scale)]
            if lo + 2 * B < NB:
                rest = m_ref[lo + 2 * B:, :]
                h, l = split2(rest[:, :NB])

                def padded(x):
                    above = [jnp.zeros((lo, 2 * NB), BF)] if lo else []
                    return jnp.concatenate(above + [x, jnp.zeros((NB - lo - B, 2 * NB), BF)], axis=0)

                wh, wl = map(padded, split2(jnp.concatenate(w, axis=0)))
                m_ref[lo + 2 * B:, :] = rest - mm(left3(h, l), jnp.concatenate([wh, wl, wh], axis=0))
            rows = []
            for t in range(T):
                terms = [wide(raw[k][t]) * row(w[k // 8], k % 8) for k in range(B)]
                sums = [sum(terms[g + 2:B:2], terms[g]) for g in range(2)]
                rows.append(nxt[t] - (sums[0] + sums[1]))


MESH = pl.DeviceIdType.MESH


def dot3(lhs, h, l):
    return mm(lhs, jnp.concatenate([h, l, h], axis=0))


def left3(h, l):
    return jnp.concatenate([h, h, l], axis=1)


def fused_body(n, fronts, cap, B, x_hbm, d_hbm, ch_hbm, cc_hbm, w_hbm, o_ref, x_ref, d_ref, ch_ref, cc_ref, w_ref, ls, out_ref, in_ref, fs, fg, a_ref, m_ref, rt_ref, rr_ref, mh_ref, ml_ref, tt_ref, xh_ref, xl_ref, th_ref, tl_ref, p_ref, l_ref, f_ref, dp_ref, dl_ref, df_ref, dr_ref, rd_ref, ss, sg, ds, dg, os, og, ps, pg, go):
    R, F = x_hbm.shape
    kids, crows, _ = ch_hbm.shape
    slots = fronts * cap
    panels = F // NB
    chunks = F // CW
    me = lax.axis_index("sub")
    mine = lax.axis_index("front")
    side = lax.rem(mine, 2)
    pos = me + side * (n - 1 - 2 * me)
    top = (n - 1) * (1 - side)
    step = 1 - 2 * side
    is_root = pos == n - 1
    is_first = pos == 0

    barrier = pltpu.get_barrier_semaphore()

    def greet_sub(k, c):
        pl.semaphore_signal(barrier, inc=1, device_id={"sub": lax.rem(me + k, n)}, device_id_type=MESH)
        return c

    def greet_front(k, c):
        pl.semaphore_signal(barrier, inc=1, device_id={"front": lax.rem(mine + k, fronts)}, device_id_type=MESH)
        return c

    lax.fori_loop(1, n, greet_sub, 0)
    lax.fori_loop(1, fronts, greet_front, 0)

    def cols_of(c):
        return pl.ds(pl.multiple_of(c * CW, CW), CW)

    def rows_of(f):
        return pl.ds(pl.multiple_of(f * cap, cap), cap)

    def post(k, c, dst_front):
        to = lax.rem(mine + k, fronts)
        return pltpu.make_async_remote_copy(
            src_ref=out_ref.at[c, rows_of(to)], dst_ref=in_ref.at[c, rows_of(dst_front)], send_sem=fs.at[c, k],
            recv_sem=fg.at[c, k], device_id={"front": to}, device_id_type=MESH)

    def load(c):
        return pltpu.make_async_copy(x_hbm.at[:, cols_of(c)], x_ref.at[c], ls.at[c])

    small = [pltpu.make_async_copy(src, dst, ls.at[chunks + i]) for i, (src, dst) in enumerate(
        ((d_hbm, d_ref), (ch_hbm, ch_ref), (cc_hbm, cc_ref), (w_hbm, w_ref)))]
    small[0].start()

    def load_all(c, cc):
        load(c).start()
        return cc

    lax.fori_loop(0, chunks, load_all, 0)
    for copy in small[1:]:
        copy.start()
    small[0].wait()
    dest = d_ref[...]
    hot = dest == lax.broadcasted_iota(jnp.int32, (fronts, R), 0)
    above = lax.broadcasted_iota(jnp.int32, (R, R), 0) < lax.broadcasted_iota(jnp.int32, (R, R), 1)
    before = mm(hot.astype(F32).astype(BF), above.astype(F32).astype(BF))
    position = jnp.sum(jnp.where(hot, before, 0.0), axis=0, keepdims=True)
    slot_of = dest.astype(F32) * cap + position
    pick = (slot_of == lax.broadcasted_iota(jnp.int32, (slots, R), 0).astype(F32)).astype(F32).astype(BF)
    pick2 = jnp.concatenate([pick, pick], axis=1)

    def route(c):
        load(c).wait()
        out_ref[c] = mm(pick2, jnp.concatenate(split2(x_ref[c]), axis=0))

    def post_rows(c):
        for odd in (1, 0):
            def one(t, cc):
                k = lax.rem(2 * t + odd - mine + fronts, fronts)

                @pl.when(k > 0)
                def _():
                    post(k, c, mine).start()
                return cc

            lax.fori_loop(0, fronts // 2, one, 0)
        in_ref[c, rows_of(mine), :] = out_ref[c, rows_of(mine), :]

    route(0)
    pl.semaphore_wait(barrier, fronts + n - 2)
    post_rows(0)

    def route_rest(c, cc):
        route(c)
        post_rows(c)
        return cc

    lax.fori_loop(1, chunks, route_rest, 0)

    for copy in small[1:]:
        copy.wait()

    def place_kids(c, cc):
        for kid in range(kids):
            h, l = split2(ch_ref[kid])
            spread = (lax.broadcasted_iota(jnp.int32, (CW, cc_ref.shape[1]), 0) + c * CW == cc_ref[kid:kid + 1, :]).astype(F32).astype(BF)
            both = lax.dot_general(jnp.concatenate([h, l], axis=0), spread, (((1,), (1,)), ((), ())), preferred_element_type=F32)
            xh_ref[c, kid * crows:(kid + 1) * crows, :] = both[:crows].astype(BF)
            xl_ref[c, kid * crows:(kid + 1) * crows, :] = both[crows:].astype(BF)
        return cc

    lax.fori_loop(0, chunks, place_kids, 0)

    ri = lax.broadcasted_iota(jnp.int32, (NB, NB), 0)
    ci = lax.broadcasted_iota(jnp.int32, (NB, NB), 1)

    def place(i, j):
        return j * (j + 1) // 2 + i

    def hop(src, dst, c, send, recv):
        return pltpu.make_async_remote_copy(
            src_ref=src.at[c], dst_ref=dst.at[c], send_sem=send.at[c], recv_sem=recv.at[c],
            device_id={"sub": lax.rem(me + step + n, n)}, device_id_type=MESH)

    def hop_block(src, c):
        return hop(src, l_ref, c, ss, sg)

    def hop_pair(src, J):
        return hop(src, dl_ref, J, ds, dg)

    def stream(copy, own, came, sums, c):
        @pl.when(is_first)
        def _():
            copy(own, c).start()

        @pl.when((pos > 0) & (pos < n - 1))
        def _():
            copy(sums, c).wait_recv()
            sums[c] = came[c] + own[c]
            copy(sums, c).start()

    def pack(ref, c, a, b):
        ref[c, :NB, :] = jnp.where(ci >= ri, a, b)
        ref[c, NB:, :] = jnp.broadcast_to(jnp.sum(jnp.where(ri == ci, b, 0.0), axis=0, keepdims=True), (8, NB))

    def gram_chunk(J, carry):
        def take(k, cc):
            post(k, J, lax.rem(mine + fronts - k, fronts)).wait_recv()
            return cc

        lax.fori_loop(1, fronts, take, 0)
        h, l = split2(in_ref[J])
        xh_ref[J, kids * crows:, :] = h
        xl_ref[J, kids * crows:, :] = l
        th_ref[J] = xh_ref[J].T
        tl_ref[J] = xl_ref[J].T

        def gram_block(I, cc):
            block = dot3(left3(th_ref[I], tl_ref[I]), xh_ref[J], xl_ref[J])
            i, j = 2 * I, 2 * J
            p_ref[place(i, j + 1)] = block[:NB, NB:]

            @pl.when(J > I)
            def _():
                p_ref[place(i, j)] = block[:NB, :NB]
                p_ref[place(i + 1, j)] = block[NB:, :NB]
                p_ref[place(i + 1, j + 1)] = block[NB:, NB:]
                stream(hop_block, p_ref, l_ref, f_ref, place(i, j))
                stream(hop_block, p_ref, l_ref, f_ref, place(i + 1, j))

            @pl.when(J == I)
            def _():
                pack(dp_ref, J, block[:NB, :NB], block[NB:, NB:])
                stream(hop_pair, dp_ref, dl_ref, df_ref, J)

            stream(hop_block, p_ref, l_ref, f_ref, place(i, j + 1))

            @pl.when(J > I)
            def _():
                stream(hop_block, p_ref, l_ref, f_ref, place(i + 1, j + 1))
            return cc

        return lax.fori_loop(0, J + 1, gram_block, carry)

    lax.fori_loop(0, chunks, gram_chunk, 0)

    def at(i, j):
        return (pl.ds(pl.multiple_of(i * NB, NB), NB), pl.ds(pl.multiple_of(j * NB, NB), NB))

    def at2(i, j):
        return (pl.ds(pl.multiple_of(i * CW, CW), CW), pl.ds(pl.multiple_of(j * CW, CW), CW))

    span = chunks // n

    def ship(Q, P):
        owner = Q // span
        return pltpu.make_async_remote_copy(
            src_ref=a_ref.at[at2(Q, P)], dst_ref=o_ref.at[at2(Q - owner * span, P)], send_sem=os.at[Q, P],
            recv_sem=og.at[Q, P], device_id={"sub": owner}, device_id_type=MESH)

    def own(Q, P):
        return pltpu.make_async_copy(a_ref.at[at2(Q, P)], o_ref.at[at2(Q - me * span, P)], os.at[Q, P])

    def ship_side(P):
        owner = P // span
        return pltpu.make_async_remote_copy(
            src_ref=a_ref.at[at(2 * P, 2 * P + 1)], dst_ref=o_ref.at[at(2 * (P - owner * span), 2 * P + 1)],
            send_sem=os.at[P, P], recv_sem=og.at[P, P], device_id={"sub": owner}, device_id_type=MESH)

    def ship_pair(P):
        return pltpu.make_async_remote_copy(
            src_ref=dr_ref.at[P], dst_ref=rd_ref.at[P], send_sem=ps.at[P], recv_sem=pg.at[P],
            device_id={"sub": P // span}, device_id_type=MESH)

    hold = chunks // 2

    def send_block(Q, P):
        @pl.when(Q // span == me)
        def _():
            own(Q, P).start()

        @pl.when(Q // span != me)
        def _():
            ship(Q, P).start()

    def send_column(P):
        def one(Q, cc):
            send_block(Q, P)
            return cc
        lax.fori_loop(0, P, one, 0)

    def send_side(P):
        @pl.when(P // span != me)
        def _():
            ship_side(P).start()

    def send_pair(P):
        @pl.when(P // span != me)
        def _():
            ship_pair(P).start()

    def serve(i, j):
        c = place(i, j)
        hop_block(p_ref, c).wait_recv()
        a_ref[at(i, j)] = p_ref[c] + l_ref[c]

    def serve_pair(P):
        hop_pair(dp_ref, P).wait_recv()
        m = dp_ref[P, :NB, :] + dl_ref[P, :NB, :]
        d = dp_ref[P, NB:, :] + dl_ref[P, NB:, :]
        mt = m.T
        for k, block in ((0, jnp.where(ci >= ri, m, mt)), (1, jnp.where(ci > ri, mt, jnp.where(ci < ri, m, d[:1])))):
            i = 2 * P + k
            wt = w_ref[:, pl.ds(pl.multiple_of(i * NB, NB), NB)]
            a_ref[at(i, i)] = block + jnp.where(ri == ci, wt * wt, 0.0)

    def factor(p):
        m_ref[:, :NB] = a_ref[at(p, p)]
        m_ref[:, NB:] = (ri == ci).astype(F32)
        factor_diag(m_ref, B)
        a_ref[at(p, p)] = jnp.where(ci >= ri, m_ref[:, :NB], 0.0)
        return jnp.where(ci <= ri, m_ref[:, NB:], 0.0)

    def keep_t(P, r0, c0, t):
        h, l = split2(t)
        tt_ref[P, r0:r0 + NB, c0:c0 + NB] = h
        tt_ref[P, r0:r0 + NB, CW + c0:CW + c0 + NB] = h
        tt_ref[P, r0:r0 + NB, 2 * CW + c0:2 * CW + c0 + NB] = l

    def supercolumn(P, carry):
        def subtract(I, cc):
            def one(Q, c3):
                a_ref[at2(I, P)] -= mm(rt_ref[Q, I], rr_ref[Q])
                return c3
            return lax.fori_loop(0, I, one, cc)

        def solve(I, cc):
            for i in range(2):
                for j in range(2):
                    serve(2 * I + i, 2 * P + j)
            subtract(I, cc)
            h, l = split2(a_ref[at2(I, P)])
            r = dot3(tt_ref[I], h, l)
            a_ref[at2(I, P)] = r
            h, l = split2(r)
            rr_ref[I] = jnp.concatenate([h, l, h], axis=0)
            rt_ref[I, P] = left3(h.T, l.T)
            return cc

        lax.fori_loop(0, P, solve, 0)

        @pl.when(P == hold)
        def _():
            pl.semaphore_wait(go, 1)

            def backlog(t, cc):
                Q = side * t + (1 - side) * (P - 1 - t)
                send_side(Q)
                send_pair(Q)

                def one(K, c3):
                    send_block(Q, K)
                    return c3
                return lax.fori_loop(Q + 1, P + 1, one, cc)
            lax.fori_loop(0, P, backlog, 0)

        @pl.when(P > hold)
        def _():
            send_column(P)

        serve(2 * P, 2 * P + 1)
        serve_pair(P)
        a_ref[at(2 * P + 1, 2 * P)] = jnp.zeros((NB, NB), F32)
        subtract(P, 0)
        p = 2 * P
        t0 = factor(p)
        h, l = split2(a_ref[at(p, p + 1)])
        th, tl = split2(t0)
        r = dot3(left3(th, tl), h, l)
        a_ref[at(p, p + 1)] = r

        @pl.when(P >= hold)
        def _():
            send_side(P)

        h, l = split2(r)
        rl = left3(h.T, l.T)
        a_ref[at(p + 1, p + 1)] -= dot3(rl, h, l)
        keep_t(P, 0, 0, t0)
        keep_t(P, 0, NB, jnp.zeros((NB, NB), F32))
        mh_ref[...], ml_ref[...] = split2(dot3(rl, th, tl))
        t1 = factor(p + 1)

        @pl.when(P // span == me)
        def _():
            own(P, P).start()

        @pl.when(P // span != me)
        def _():
            pack(dr_ref, P, a_ref[at(p, p)], a_ref[at(p + 1, p + 1)].T)

        @pl.when(P >= hold)
        def _():
            send_pair(P)

        keep_t(P, NB, NB, t1)
        th, tl = split2(t1)
        keep_t(P, NB, 0, -dot3(left3(th, tl), mh_ref[...], ml_ref[...]))
        return carry

    def over_blocks(lo, hi, fn, pair):
        def row(Q, c):
            def one(P, cc):
                fn(Q, P)
                return cc
            pair(Q)
            return lax.fori_loop(Q + 1, chunks, one, c)
        lax.fori_loop(lo, hi, row, 0)

    @pl.when(is_root)
    def _():
        lax.fori_loop(0, chunks, supercolumn, 0)

        def sent(Q, P):
            @pl.when(Q // span != me)
            def _():
                ship(Q, P).wait_send()

            @pl.when(Q // span == me)
            def _():
                own(Q, P).wait()

        def sent_pair(P):
            @pl.when(P // span != me)
            def _():
                ship_side(P).wait_send()
                ship_pair(P).wait_send()

            @pl.when(P // span == me)
            def _():
                own(P, P).wait()

        over_blocks(0, chunks, sent, sent_pair)

    @pl.when(jnp.logical_not(is_root))
    def _():
        def sent(c, lo, hi):
            def off(i, c3):
                hop_block(f_ref, place(i, 2 * c)).wait_send()
                hop_block(f_ref, place(i, 2 * c + 1)).wait_send()
                return c3
            lax.fori_loop(lo, hi, off, 0)

        def sent_diag(c):
            hop_pair(df_ref, c).wait_send()
            hop_block(f_ref, place(2 * c, 2 * c + 1)).wait_send()

        def whole(c, cc):
            sent(c, 0, 2 * c)
            sent_diag(c)
            return cc

        lax.fori_loop(0, chunks - 1, whole, 0)
        sent(chunks - 1, 0, panels - 2 - 0)

        @pl.when(is_first)
        def _():
            pl.semaphore_signal(go, inc=1, device_id={"front": mine + 1 - 2 * side}, device_id_type=MESH)

        sent(chunks - 1, panels - 2 - 0, panels - 2)
        sent_diag(chunks - 1)

        def came(Q, P):
            ship(Q, P).wait_recv()

        def came_pair(P):
            ship_side(P).wait_recv()
            ship_pair(P).wait_recv()
            k = 2 * (P - me * span)
            m = rd_ref[P, :NB, :]
            a_ref[at(2 * P, 2 * P)] = jnp.where(ci >= ri, m, 0.0)
            a_ref[at(2 * P + 1, 2 * P + 1)] = jnp.where(ci > ri, m.T, jnp.where(ci == ri, rd_ref[P, NB:NB + 1, :], 0.0))
            both = [pltpu.make_async_copy(a_ref.at[at(2 * P + i, 2 * P + i)], o_ref.at[at(k + i, 2 * P + i)], sem)
                    for i, sem in enumerate((ps.at[P], os.at[P, P]))]
            for copy in both:
                copy.start()
            for copy in both:
                copy.wait()

        over_blocks(me * span, me * span + span, came, came_pair)


    def sent_rows(c, cc):
        def one(k, c3):
            post(k, c, mine).wait_send()
            return c3
        return lax.fori_loop(1, fronts, one, cc)

    lax.fori_loop(0, chunks, sent_rows, 0)


def local(row_values, front_of_row, child_factors, child_columns, damping, B=16):
    fronts, n = lax.axis_size("front"), lax.axis_size("sub")
    rows_held, F = row_values.shape
    cap = -(-(2 * rows_held // fronts) // 8) * 8
    K = fronts * cap + child_factors.shape[0] * child_factors.shape[1]
    panels, chunks = F // NB, F // CW
    total = panels * (panels + 1) // 2
    DMA = pltpu.SemaphoreType.DMA
    out = pl.pallas_call(
        functools.partial(fused_body, n, fronts, cap, B),
        out_shape=jax.ShapeDtypeStruct((F // n, F), F32),
        in_specs=[pl.BlockSpec(memory_space=pltpu.HBM)] * 5,
        out_specs=pl.BlockSpec(memory_space=pltpu.HBM),
        scratch_shapes=[
            pltpu.VMEM((chunks, rows_held, CW), F32),
            pltpu.VMEM((1, rows_held), jnp.int32),
            pltpu.VMEM(child_factors.shape, F32),
            pltpu.VMEM(child_columns.shape, jnp.int32),
            pltpu.VMEM(damping.shape, F32),
            DMA((chunks + 4,)),
            pltpu.VMEM((chunks, fronts * cap, CW), F32),
            pltpu.VMEM((chunks, fronts * cap, CW), F32),
            DMA((chunks, fronts)),
            DMA((chunks, fronts)),
            pltpu.VMEM((F, F), F32),
            pltpu.VMEM((NB, 2 * NB), F32),
            pltpu.VMEM((chunks, chunks, CW, 3 * CW), BF),
            pltpu.VMEM((chunks, 3 * CW, CW), BF),
            pltpu.VMEM((NB, NB), BF),
            pltpu.VMEM((NB, NB), BF),
            pltpu.VMEM((chunks, CW, 3 * CW), BF),
            pltpu.VMEM((chunks, K, CW), BF),
            pltpu.VMEM((chunks, K, CW), BF),
            pltpu.VMEM((chunks, CW, K), BF),
            pltpu.VMEM((chunks, CW, K), BF),
        ] + [pltpu.VMEM((total, NB, NB), F32)] * 3 + [pltpu.VMEM((chunks, NB + 8, NB), F32)] * 5
        + [DMA((total,))] * 2 + [DMA((chunks,))] * 2 + [DMA((chunks, chunks))] * 2 + [DMA((chunks,))] * 2 + [pltpu.SemaphoreType.REGULAR],
        compiler_params=pltpu.CompilerParams(
            vmem_limit_bytes=60 << 20, collective_id=0, has_side_effects=True),
        name="merge",
    )(row_values, front_of_row.reshape(1, rows_held), child_factors, child_columns, damping)
    held = F // n
    below = lax.axis_index("sub") * held + lax.broadcasted_iota(jnp.int32, (held, F), 0) > lax.broadcasted_iota(jnp.int32, (held, F), 1)
    return jnp.where(below, 0.0, out)[None]


def solution(mesh):
    in_specs = (
        P(("front", "sub"), None),
        P(("front", "sub"), None),
        P("front", "sub", None),
        P("front", None),
        P("front", None),
    )
    out_specs = P("front", "sub", None)
    return jax.shard_map(local, mesh=mesh, in_specs=in_specs, out_specs=out_specs, check_vma=False)
```
